128 devices in a mesh: pts: 16 (over z_hi, x, core), wlk: 8 (over z_lo, y).
Axes of the slice: x: 4, y: 4, z: 4 (z_hi: 2, z_lo: 2; z = z_hi * 2 + z_lo), core: 2. Of those that a mesh axis runs over, the one named last changes fastest.
Arguments:
- green_half: bfloat16 [16, 400, 2400], P('wlk'), may hold values from -6 to 6
- collocation: bfloat16 [2400, 9600], P('wlk', 'pts'), may hold values from -0.125 to 0.125
- occupied: bfloat16 [9600, 400], P('pts'), may hold values from -0.0029296875 to 0.0029296875
- kernel: bfloat16 [9600, 9600], P('pts'), may hold values from 0 to 16, as said below
Outputs:
- potential: float32 [16, 9600], P('wlk', 'pts')
- coulomb_energy: float32 [16], P('wlk')
- exchange_energy: float32 [16], P('wlk')
The draws below stay inside these ranges and needn't reach their ends.
Inputs may be any that keep to these rules, and one draw needn't show every extreme that they name: kernel is symmetric and positive definite: kernel[p, q] equals kernel[q, p].
All inputs are finite; a program needn't handle non-finite values.
Results may differ from the reference program's by a relative error of at most 0.008.
Values may be sent and summed in bfloat16 or wider, within the bound.
A program may use at most 192 MiB of HBM per device.

```python
import jax
import jax.numpy as jnp
from jax import lax

ORB = 2400
ELEC = 400
RANK = 9600
W = 16


def draw_kernel(key, part):
    point_spots = jax.random.uniform(jax.random.fold_in(key, 3), (RANK, 3), jnp.float32, 0.0, 1.0)
    length = (10.0 / RANK) ** (1.0 / 3.0)
    squared = jnp.zeros((RANK, RANK), jnp.float32)
    for column in range(3):
        offset = point_spots[:, column][:, None] - point_spots[:, column][None, :]
        squared = squared + offset * offset
    distance = jnp.sqrt(squared)
    values = 6.0 * jnp.exp(-distance / length) + 1.5 * jnp.eye(RANK, dtype=jnp.float32)
    return values.astype(jnp.bfloat16)


def block_scale(own_key, extent, split, smallest, largest):
    level, own = 1.0, jax.random.fold_in(own_key, 6)
    for axis_at, shards_of in split:
        draws = jnp.exp(jax.random.uniform(jax.random.fold_in(own, axis_at), (shards_of,), jnp.float32, smallest / len(split), largest / len(split)))
        level = level * jnp.repeat(draws, extent[axis_at] // shards_of).reshape([-1 if axis == axis_at else 1 for axis in range(len(extent))])
    return level


def noise(rng, shape, scale, limit, split=(), held_as=jnp.bfloat16):
    values = scale * jax.random.normal(rng, shape, jnp.float32)
    if split:
        values = values * block_scale(rng, shape, split, -0.22, 0.18)
    return jnp.clip(values, -limit, limit).astype(held_as)


def setup_inputs(seed: int = 0) -> dict:
    arg_keys = jax.random.split(jax.random.key(seed), 5)
    return {
        "green_half": noise(arg_keys[0], (W, ELEC, ORB), 1.0, 6.0, ((0, 8),)),
        "collocation": noise(arg_keys[1], (ORB, RANK), ORB ** -0.5, 0.125, ((0, 8), (1, 16))),
        "occupied": noise(arg_keys[2], (RANK, ELEC), (RANK * ELEC) ** -0.5, 0.0029296875, ((0, 16),)),
        "kernel": draw_kernel(jax.random.fold_in(arg_keys[4], 71), 0),
    }


def reference(green_half, collocation, occupied, kernel):
    kernel_float = kernel.astype(jnp.float32)

    def one_walker(green_one):
        theta = jnp.dot(green_one, collocation, preferred_element_type=jnp.float32).astype(jnp.bfloat16)
        density = jnp.sum(theta.astype(jnp.float32) * occupied.T.astype(jnp.float32), axis=0)
        density_b = density.astype(jnp.bfloat16)
        potential = jnp.dot(kernel, density_b, preferred_element_type=jnp.float32)
        coulomb = 0.5 * jnp.sum(density * potential)
        cross = jnp.dot(theta.T, occupied.T, preferred_element_type=jnp.float32)
        exchange = -0.5 * jnp.sum(kernel_float * cross * cross.T)
        return potential, coulomb, exchange

    potential, coulomb, exchange = lax.map(one_walker, green_half)
    return potential, coulomb, exchange
```

```python
import jax
import jax.numpy as jnp
from jax import lax
from jax.experimental import pallas as pl
from jax.experimental.pallas import tpu as pltpu
from jax.sharding import PartitionSpec as P

MESH = pl.DeviceIdType.MESH
F32, BF16 = jnp.float32, jnp.bfloat16

ELEC = 400
PTS = 600
PAD = 640
ROWS = 608
DEEP = 300
DEEP_PAD = 304
GROUPS = 8
C_CUT = 160
KCH = 160
CHUNK = ((0, 384), (384, 256))
STEPS = ((0, 3), (3, 5))
FLOWS = 96


def dot(a, b):
    return jnp.dot(a, b, preferred_element_type=F32)


def body(green, colloc, occ, kmat, pot_out, sum_out,
         cin, oin, gv, g8, kst, kb, cbuf, acc, ttown, ttbuf, tp, op, otown, otbuf,
         trans, dens, dbuf, ebuf, exch, pot, local_sem, send, recv, d_send, d_recv, e_send, e_recv):
    a, g = lax.axis_index("pts"), lax.axis_index("wlk")
    zh, x, c = a // 8, (a // 2) % 4, a % 2
    zl, y = g // 4, g % 4
    z = zh * 2 + zl
    is_same = zh == zl
    is_cross = zh != zl
    same = is_same.astype(jnp.int32)

    def at(zz, xx, cc, yy):
        return {"pts": (zz // 2) * 8 + xx * 2 + cc, "wlk": (zz % 2) * 4 + yy}

    sib = at(z, x, 1 - c, y)
    right, left = at(z, (x + 1) % 4, c, y), at(z, (x + 3) % 4, c, y)
    up, down = at(z, x, c, (y + 1) % 4), at(z, x, c, (y + 3) % 4)
    zmate = at(zh * 2 + 1 - zl, x, c, y)
    xmate = at(3 - z, x, c, y)
    lanes = tuple(pl.ds(pl.multiple_of(2 * start + c * size, 128), size) for start, size in CHUNK)
    cols = tuple(pl.ds(start, size) for start, size in CHUNK)
    numbers = iter(range(FLOWS))

    def flow(src, dst, dev):
        f = next(numbers)
        return pltpu.make_async_remote_copy(
            src_ref=src, dst_ref=dst, send_sem=send.at[f], recv_sem=recv.at[f],
            device_id=dev, device_id_type=MESH)

    def start(*copies):
        for cp in copies:
            cp.start()

    load_c = pltpu.make_async_copy(colloc, cin, local_sem.at[0])
    load_o = pltpu.make_async_copy(occ, oin, local_sem.at[1])
    load_g = [pltpu.make_async_copy(green.at[w], gv.at[pl.ds(w * ELEC, ELEC)], local_sem.at[2 + w]) for w in range(2)]
    pieces = [(s, min(KCH, PTS - s)) for s in range(0, PTS, KCH)]
    load_k = [pltpu.make_async_copy(kmat.at[pl.ds(s, n)], kst.at[i % 2, pl.ds(0, n)], local_sem.at[4 + i])
              for i, (s, n) in enumerate(pieces)]
    start(load_c, load_o)

    plane = z * 8 + x * 2 + c

    def plane_dev(r):
        q = (plane + r) % 32
        return at(q // 8, (q // 2) % 4, q % 2, y)

    barrier = pltpu.get_barrier_semaphore()
    for dev in (up, down):
        pl.semaphore_signal(barrier, inc=1, device_id=dev, device_id_type=MESH)

    def greet(r, carry):
        pl.semaphore_signal(barrier, inc=1, device_id=plane_dev(r), device_id_type=MESH)
        return carry

    lax.fori_loop(1, 32, greet, 0)
    cbuf[g, :, pl.ds(PAD - 128, 128)] = jnp.zeros((DEEP_PAD, 128), BF16)
    cbuf[g, pl.ds(DEEP_PAD - 16, 16), :] = jnp.zeros((16, PAD), BF16)
    load_c.wait()
    cbuf[g, pl.ds(0, DEEP), pl.ds(0, PTS)] = cin[...]
    start(*load_g)
    load_o.wait()
    otown[:, pl.ds(PAD - 128, 128)] = jnp.zeros((ELEC, 128), BF16)
    otown[:, pl.ds(0, PTS)] = oin[...]

    @pl.when(is_same)
    def _():
        for h in range(2):
            otbuf[0, :, lanes[h]] = otown[:, cols[h]]

    pl.semaphore_wait(barrier, 33)

    def slot(zlo, yy):
        return zlo * 4 + yy

    def c_flow(k, h, dev, first=0, count=DEEP_PAD):
        ref = cbuf.at[k, pl.ds(first, count), cols[h]]
        return flow(ref, ref, dev)

    own_k, mate_k = slot(zl, y), slot(1 - zl, y)
    dn, un, on = (y + 3) % 4, (y + 1) % 4, (y + 2) % 4
    c_z, c_own, c_mate, c_far, c_matefar = [], [], [], [], []
    for h in range(2):
        c_z.append(c_flow(own_k, h, zmate))
        c_own.append((c_flow(own_k, h, up), c_flow(own_k, h, down)))
        c_mate.append((c_flow(mate_k, h, up), c_flow(mate_k, h, down)))
        c_far.append((c_flow(slot(zl, dn), h, up, 0, C_CUT),
                      c_flow(slot(zl, un), h, down, C_CUT, DEEP_PAD - C_CUT)))
        c_matefar.append((c_flow(slot(1 - zl, dn), h, up, 0, C_CUT),
                          c_flow(slot(1 - zl, un), h, down, C_CUT, DEEP_PAD - C_CUT)))
    start(c_own[0][0], c_own[0][1], c_z[0], c_z[1])

    def o_block(i, h):
        return otbuf.at[i, :, lanes[h]]

    o_xx = [flow(otown.at[:, cols[h]], o_block(0, h), xmate) for h in range(2)]
    o_right = [flow(o_block(0, h), o_block(1, h), right) for h in range(2)]
    o_left = [flow(o_block(0, h), o_block(2, h), left) for h in range(2)]
    o_sib = [flow(o_block(0, h), o_block(0, h), sib) for h in range(2)]
    o_far = [flow(o_block(1, 0), o_block(3, 0), right), flow(o_block(2, 1), o_block(3, 1), left)]
    o_relay = [[flow(o_block(i, h), o_block(i, h), sib) for h in range(2)] for i in (1, 2, 3)]
    o_first = [o_right[0], o_left[0], o_right[1], o_left[1]] + o_sib

    @pl.when(is_cross)
    def _():
        start(*o_xx)

    @pl.when(is_same)
    def _():
        start(*o_first)

    for cp in load_g:
        cp.wait()
    start(load_k[0], load_k[1])

    def cut_green(r, carry):
        rows = pl.ds(pl.multiple_of(r * 80, 16), 80)
        piece = gv[rows, :]
        for k in range(GROUPS):
            part = piece[:, k * DEEP:(k + 1) * DEEP]
            g8[k, rows, pl.ds(0, DEEP_PAD)] = jnp.concatenate([part, jnp.zeros((80, DEEP_PAD - DEEP), BF16)], axis=1)
        return carry

    lax.fori_loop(0, 10, cut_green, 0)

    def add_theta(k, h, first=False):
        part = dot(g8[k, :, pl.ds(0, DEEP_PAD)], cbuf[k, :, cols[h]])
        if first:
            acc[:, cols[h]] = part
        else:
            acc[:, cols[h]] += part

    def cut_kernel(i):
        s, n = pieces[i]
        load_k[i].wait()

        def rows_at(r, carry):
            rows = pl.ds(pl.multiple_of(r * 16, 16), 16)
            out = pl.ds(pl.multiple_of(s + r * 16, 16), 16)
            for b in range(16):
                j, core = b // 2, b % 2
                kb[j, out, pl.ds(core * 384, 384)] = kst[i % 2, rows, pl.ds(b * PTS, 384)]
                part = kst[i % 2, rows, pl.ds(b * PTS + 384, PTS - 384)]
                kb[j, out, pl.ds(768 + core * 256, 256)] = jnp.concatenate(
                    [part, jnp.zeros((16, PAD - PTS), BF16)], axis=1)
            return carry

        lax.fori_loop(0, (n + 15) // 16, rows_at, 0)
        if i + 2 < len(pieces):
            load_k[i + 2].start()

    add_theta(own_k, 0, True)
    add_theta(own_k, 1, True)

    c_z[0].wait_recv()
    start(*c_mate[0])
    c_own[0][0].wait_recv()
    c_far[0][0].start()
    c_own[0][1].wait_recv()
    c_far[0][1].start()
    start(*c_own[1])
    add_theta(mate_k, 0)
    add_theta(slot(zl, dn), 0)
    add_theta(slot(zl, un), 0)
    c_z[1].wait_recv()
    start(*c_mate[1])
    cut_kernel(0)
    c_mate[0][0].wait_recv()
    c_matefar[0][0].start()
    c_mate[0][1].wait_recv()
    c_matefar[0][1].start()
    add_theta(slot(1 - zl, dn), 0)
    add_theta(slot(1 - zl, un), 0)

    @pl.when(is_cross)
    def _():
        for cp in o_xx:
            cp.wait_recv()
        start(*o_first)

    add_theta(mate_k, 1)
    c_far[0][0].wait_recv()
    c_far[0][1].wait_recv()
    add_theta(slot(zl, on), 0)
    c_own[1][0].wait_recv()
    c_far[1][0].start()
    c_own[1][1].wait_recv()
    c_far[1][1].start()
    add_theta(slot(zl, dn), 1)
    c_matefar[0][0].wait_recv()
    c_matefar[0][1].wait_recv()
    add_theta(slot(1 - zl, on), 0)

    def t_block(i, h):
        return ttbuf.at[i, :, lanes[h]]

    def t_flows(count, make):
        return [[make(w, h) for h in range(2)] for w in range(count)]

    t_z = t_flows(2, lambda w, h: flow(ttown.at[w, :, cols[h]], t_block(2 + w, h), zmate))
    t_xx = t_flows(2, lambda w, h: flow(ttown.at[w, :, cols[h]], t_block(w, h), xmate))
    t_sib = t_flows(2, lambda w, h: flow(t_block(w, h), t_block(w, h), sib))
    t_sibz = t_flows(2, lambda w, h: flow(t_block(2 + w, h), t_block(2 + w, h), sib))
    t_right = t_flows(2, lambda w, h: flow(t_block(w * (1 + same), h), t_block(4 + w, h), right))
    t_left = t_flows(2, lambda w, h: flow(t_block(same + w * (1 + same), h), t_block(6 + w, h), left))
    low_r = (x + 1) % 4 < 2
    low_l = (x + 3) % 4 < 2
    go_r = 4 + jnp.where(is_same & jnp.logical_not(low_r), 1, 0)
    go_l = 6 + jnp.where(is_same & low_l, 0, 1)
    t_far = [[flow(t_block(go_r, h), t_block(8, h), right) for h in range(2)],
             [flow(t_block(go_l, h), t_block(9, h), left) for h in range(2)]]
    t_relay = [[flow(t_block(i, h), t_block(i, h), sib) for h in range(2)] for i in range(4, 10)]

    def publish(h):
        for w in range(2):
            t = acc[pl.ds(w * ELEC, ELEC), cols[h]].astype(BF16)
            ttown[w, :, cols[h]] = t

            @pl.when(is_same)
            def _():
                ttbuf[w, :, lanes[h]] = t

            dens[pl.ds(w, 1), cols[h]] = jnp.sum(
                t.astype(F32) * otown[:, cols[h]].astype(F32), axis=0, keepdims=True)

        @pl.when(is_cross)
        def _():
            start(t_xx[0][h], t_z[0][h], t_xx[1][h], t_z[1][h])

        @pl.when(is_same)
        def _():
            start(t_z[0][h], t_right[0][h], t_left[0][h], t_z[1][h], t_sib[0][h], t_sib[1][h])

    publish(0)

    c_mate[1][0].wait_recv()
    c_matefar[1][0].start()
    c_mate[1][1].wait_recv()
    c_matefar[1][1].start()
    add_theta(slot(zl, un), 1)
    add_theta(slot(1 - zl, dn), 1)
    add_theta(slot(1 - zl, un), 1)

    for h in range(2):
        o_right[h].wait_recv()
        o_left[h].wait_recv()
    start(*o_far, *o_relay[0], *o_relay[1])
    trans[...] = jnp.zeros_like(trans)

    c_far[1][0].wait_recv()
    c_far[1][1].wait_recv()
    add_theta(slot(zl, on), 1)
    c_matefar[1][0].wait_recv()
    c_matefar[1][1].wait_recv()
    add_theta(slot(1 - zl, on), 1)
    publish(1)

    dbuf[a] = dens[...].astype(BF16).astype(F32)

    def d_flow(r):
        return pltpu.make_async_remote_copy(
            src_ref=dbuf.at[a], dst_ref=dbuf.at[a], send_sem=d_send.at[r], recv_sem=d_recv.at[r],
            device_id={"pts": (a + r) % 16, "wlk": g}, device_id_type=MESH)

    def d_start(r, carry):
        d_flow(r).start()
        return carry

    def d_wait(r, carry):
        d_flow(r).wait()
        return carry

    lax.fori_loop(1, 16, d_start, 0)

    def turned(src, size):
        trans[pl.ds(0, ELEC), pl.ds(0, size)] = src.astype(F32)
        return jnp.swapaxes(trans[:, pl.ds(0, size)], 0, 1).astype(BF16)

    def turn(side, h):
        tp[side, cols[h], :] = turned(ttbuf[side, :, lanes[h]], CHUNK[h][1])

    def potential():
        pot[...] = jnp.zeros_like(pot)

        def add_chip(j, carry):
            one, two = dbuf[2 * j].astype(BF16), dbuf[2 * j + 1].astype(BF16)
            both = jnp.concatenate([one[:, :384], two[:, :384], one[:, 384:], two[:, 384:]], axis=1)
            pot[...] += lax.dot_general(both, kb[j], (((1,), (1,)), ((), ())), preferred_element_type=F32)
            return carry

        lax.fori_loop(0, 8, add_chip, 0)
        pot_out[...] = pot[:, pl.ds(0, PTS)]

    exch[...] = jnp.zeros_like(exch)

    def unit(tt, side, ot, chip, weight, h):
        left_t = tp[side, pl.ds(0, ROWS), pl.ds(0, ELEC)]
        left_o = op[pl.ds(0, ROWS), pl.ds(0, ELEC)]

        def step(n, carry):
            part = pl.ds(pl.multiple_of(n * 256, 256), 256)
            near = dot(left_t, otbuf[ot, :, part])
            away = dot(left_o, ttbuf[tt, :, part])
            terms = kb[chip, :, part].astype(F32) * near * away
            return carry + terms.reshape(ROWS // 8, 8, 256).sum(axis=0)

        total = lax.fori_loop(*STEPS[h], step, jnp.zeros((8, 256), F32))
        exch[side] += weight * total

    far_zh = jnp.where(is_same, zh, 1 - zh) * 4
    chip_0, chip_1, chip_2, chip_3 = (far_zh + (x + d) % 4 for d in (0, 3, 1, 2))
    cross2 = 2 * (1 - same)
    self_weight = jnp.where(is_same, 1.0, 2.0)
    far_side = jnp.where(is_cross | (x >= 2), 2, 0)
    units = {
        0: (cross2, 0, chip_0, self_weight), 1: (cross2 + 1, 0, chip_0, self_weight),
        2: (2, 0, chip_0, self_weight), 3: (3, 0, chip_0, self_weight),
        4: (cross2, 1, chip_1, 2.0), 5: (3 - same, 1, chip_1, 2.0),
        6: (cross2 + same, 2, chip_2, 2.0), 7: (3, 2, chip_2, 2.0),
        8: (far_side, 3, chip_3, 2.0), 9: (far_side + 1, 3, chip_3, 2.0),
    }

    def run(tt, h):
        unit(tt, *units[tt], h)

    def pass_on(w, h):
        @pl.when(is_same)
        def _():
            t_z[w][h].wait_recv()
            start(t_right[1][h] if w == 0 else t_left[1][h], t_sibz[w][h])

        @pl.when(is_cross)
        def _():
            t_xx[w][h].wait_recv()
            start(t_right[w][h], t_left[w][h], t_sib[w][h])
            t_z[w][h].wait_recv()

        turn(2 + w, h)

    def arrive(first, second, h):
        t_right[first][h].wait_recv()
        t_relay[first][h].start()
        t_left[second][h].wait_recv()
        t_relay[2 + second][h].start()

    op[...] = turned(otown[...], PAD)

    @pl.when(is_same)
    def _():
        for w in range(2):
            for h in range(2):
                turn(w, h)

    cut_kernel(1)
    pass_on(0, 0)
    cut_kernel(2)
    cut_kernel(3)
    kb[:, pl.ds(PTS, ROWS - PTS), :] = jnp.zeros((8, ROWS - PTS, 2 * PAD), BF16)
    o_far[0].wait_recv()
    o_far[1].wait_recv()
    start(*o_relay[2])

    pass_on(1, 0)
    for h in range(2):
        o_sib[h].wait_recv()

    @pl.when(is_same)
    def _():
        for h in range(2):
            t_sib[0][h].wait_recv()
            run(0, h)

    arrive(0, 0, 0)
    pass_on(0, 1)

    @pl.when(is_cross)
    def _():
        for h in range(2):
            t_sib[0][h].wait_recv()
            run(0, h)

    pass_on(1, 1)
    arrive(1, 1, 0)
    start(t_far[0][0], t_far[1][0])

    for h in range(2):
        t_sib[1][h].wait_recv()
    run(1, 0)
    for i in (0, 1):
        for h in range(2):
            o_relay[i][h].wait_recv()
    t_relay[0][0].wait_recv()
    run(4, 0)
    t_relay[2][0].wait_recv()
    run(6, 0)
    arrive(0, 0, 1)
    t_relay[1][0].wait_recv()
    run(5, 0)
    t_relay[3][0].wait_recv()
    run(7, 0)
    arrive(1, 1, 1)
    start(t_far[0][1], t_far[1][1])
    run(1, 1)
    t_relay[0][1].wait_recv()
    run(4, 1)
    t_relay[2][1].wait_recv()
    run(6, 1)

    @pl.when(is_same)
    def _():
        for w in range(2):
            for h in range(2):
                t_sibz[w][h].wait_recv()
                run(2 + w, h)

    lax.fori_loop(1, 16, d_wait, 0)
    potential()

    t_far[0][0].wait_recv()
    t_relay[4][0].start()
    t_far[1][0].wait_recv()
    t_relay[5][0].start()
    t_relay[1][1].wait_recv()
    run(5, 1)
    t_relay[3][1].wait_recv()
    run(7, 1)
    for h in range(2):
        o_relay[2][h].wait_recv()
    t_relay[4][0].wait_recv()
    run(8, 0)
    t_relay[5][0].wait_recv()
    run(9, 0)
    t_far[0][1].wait_recv()
    t_relay[4][1].start()
    t_far[1][1].wait_recv()
    t_relay[5][1].start()
    t_relay[4][1].wait_recv()
    run(8, 1)
    t_relay[5][1].wait_recv()
    run(9, 1)

    row = lax.broadcasted_iota(jnp.int32, (8, 128), 0)
    tile = jnp.zeros((8, 128), F32)
    for side in range(4):
        tile = jnp.where(row == (zl * 2 + side) % 4, -0.5 * jnp.sum(exch[side]), tile)
    for w in range(2):
        tile = jnp.where(row == 4 + zl * 2 + w,
                         0.5 * jnp.sum(dens[pl.ds(w, 1), pl.ds(0, PTS)] * pot[pl.ds(w, 1), pl.ds(0, PTS)]), tile)
    ebuf[plane] = tile

    def e_flow(r):
        return pltpu.make_async_remote_copy(
            src_ref=ebuf.at[plane], dst_ref=ebuf.at[plane], send_sem=e_send.at[r], recv_sem=e_recv.at[r],
            device_id=plane_dev(r), device_id_type=MESH)

    def e_start(r, carry):
        e_flow(r).start()
        return carry

    def e_wait(r, carry):
        e_flow(r).wait()
        return carry

    lax.fori_loop(1, 32, e_start, 0)

    for pairs in (c_own, c_mate, c_far, c_matefar, t_z, t_right, t_left, t_sib, t_far, t_relay, o_relay):
        for pair in pairs:
            for cp in pair:
                cp.wait_send()
    for cp in c_z + o_first + o_far:
        cp.wait_send()

    @pl.when(is_cross)
    def _():
        for cp in o_xx + t_xx[0] + t_xx[1]:
            cp.wait_send()

    @pl.when(is_same)
    def _():
        for cp in t_sibz[0] + t_sibz[1]:
            cp.wait_send()

    lax.fori_loop(1, 32, e_wait, 0)
    sum_out[...] = ebuf[...].sum(axis=0)


def finish(pot, total, pot_out, cou_out, exc_out):
    zl = lax.axis_index("wlk") // 4
    pot_out[...] = pot[...]
    row = lax.broadcasted_iota(jnp.int32, (8, 128), 0)
    for w in range(2):
        exc_out[w] = jnp.sum(jnp.where(row == zl * 2 + w, total[...], 0.0)) * (1.0 / 128)
        cou_out[w] = jnp.sum(jnp.where(row == 4 + zl * 2 + w, total[...], 0.0)) * (1.0 / 128)


def local(green_half, collocation, occupied, kernel):
    any_space = pl.BlockSpec(memory_space=pl.ANY)
    vmem = pltpu.VMEM
    in_vmem, in_smem = pl.BlockSpec(memory_space=vmem), pl.BlockSpec(memory_space=pltpu.SMEM)
    pot, total = pl.pallas_call(
        body,
        out_shape=(jax.ShapeDtypeStruct((2, PTS), F32), jax.ShapeDtypeStruct((8, 128), F32)),
        in_specs=[any_space] * 4,
        out_specs=(in_vmem, in_vmem),
        scratch_shapes=[
            vmem((DEEP, PTS), BF16),
            vmem((ELEC, PTS), BF16),
            vmem((2 * ELEC, 8 * DEEP), BF16),
            vmem((GROUPS, 2 * ELEC, 384), BF16),
            vmem((2, KCH, 16 * PTS), BF16),
            vmem((8, ROWS, 2 * PAD), BF16),
            vmem((GROUPS, DEEP_PAD, PAD), BF16),
            vmem((2 * ELEC, PAD), F32),
            vmem((2, ELEC, PAD), BF16),
            vmem((10, ELEC, 2 * PAD), BF16),
            vmem((4, PAD, 512), BF16),
            vmem((PAD, 512), BF16),
            vmem((ELEC, PAD), BF16),
            vmem((4, ELEC, 2 * PAD), BF16),
            vmem((512, PAD), F32),
            vmem((2, PAD), F32),
            vmem((16, 2, PAD), F32),
            vmem((32, 8, 128), F32),
            vmem((4, 8, 256), F32),
            vmem((2, ROWS), F32),
            pltpu.SemaphoreType.DMA((8,)),
            pltpu.SemaphoreType.DMA((FLOWS,)),
            pltpu.SemaphoreType.DMA((FLOWS,)),
            pltpu.SemaphoreType.DMA((16,)),
            pltpu.SemaphoreType.DMA((16,)),
            pltpu.SemaphoreType.DMA((32,)),
            pltpu.SemaphoreType.DMA((32,)),
        ],
        compiler_params=pltpu.CompilerParams(
            collective_id=0, has_side_effects=True, vmem_limit_bytes=67_000_000),
    )(green_half, collocation, occupied.T, kernel)
    return pl.pallas_call(
        finish,
        out_shape=(jax.ShapeDtypeStruct((2, PTS), F32), jax.ShapeDtypeStruct((2,), F32), jax.ShapeDtypeStruct((2,), F32)),
        in_specs=[in_vmem, in_vmem],
        out_specs=(in_vmem, in_smem, in_smem),
    )(pot, total)


def solution(mesh):
    placed = (P("wlk", None, None), P("wlk", "pts"), P("pts", None), P("pts", None))
    return jax.shard_map(
        local,
        mesh=mesh,
        in_specs=placed,
        out_specs=(P("wlk", "pts"), P("wlk"), P("wlk")),
        check_vma=False,
    )
```

```python
import jax
import jax.numpy as jnp
from jax import lax
from jax.experimental import pallas as pl
from jax.experimental.pallas import tpu as pltpu
from jax.sharding import PartitionSpec as P

MESH = pl.DeviceIdType.MESH
F32, BF16 = jnp.float32, jnp.bfloat16

ELEC = 400
PTS = 600
PAD = 640
ROWS = 608
DEEP = 300
DEEP_PAD = 304
GROUPS = 8
C_CUT = 160
KCH = 160
CHUNK = ((0, 256), (256, 384))
STEPS = ((0, 2), (2, 5))
FLOWS = 96


def dot(a, b):
    return jnp.dot(a, b, preferred_element_type=F32)


def body(green, colloc, occ, kmat, pot_out, sum_out,
         cin, oin, gv, g8, kst, kb, cbuf, acc, ttown, ttbuf, tp, op, otown, otbuf,
         trans, dens, dbuf, ebuf, exch, pot, local_sem, send, recv, d_send, d_recv, e_send, e_recv):
    a, g = lax.axis_index("pts"), lax.axis_index("wlk")
    zh, x, c = a // 8, (a // 2) % 4, a % 2
    zl, y = g // 4, g % 4
    z = zh * 2 + zl
    is_same = zh == zl
    is_cross = zh != zl
    same = is_same.astype(jnp.int32)

    def at(zz, xx, cc, yy):
        return {"pts": (zz // 2) * 8 + xx * 2 + cc, "wlk": (zz % 2) * 4 + yy}

    sib = at(z, x, 1 - c, y)
    right, left = at(z, (x + 1) % 4, c, y), at(z, (x + 3) % 4, c, y)
    up, down = at(z, x, c, (y + 1) % 4), at(z, x, c, (y + 3) % 4)
    zmate = at(zh * 2 + 1 - zl, x, c, y)
    xmate = at(3 - z, x, c, y)
    lanes = tuple(pl.ds(pl.multiple_of(2 * start + c * size, 128), size) for start, size in CHUNK)
    cols = tuple(pl.ds(start, size) for start, size in CHUNK)
    numbers = iter(range(FLOWS))

    def flow(src, dst, dev):
        f = next(numbers)
        return pltpu.make_async_remote_copy(
            src_ref=src, dst_ref=dst, send_sem=send.at[f], recv_sem=recv.at[f],
            device_id=dev, device_id_type=MESH)

    def start(*copies):
        for cp in copies:
            cp.start()

    load_c = pltpu.make_async_copy(colloc, cin, local_sem.at[0])
    load_o = pltpu.make_async_copy(occ, oin, local_sem.at[1])
    load_g = [pltpu.make_async_copy(green.at[w], gv.at[pl.ds(w * ELEC, ELEC)], local_sem.at[2 + w]) for w in range(2)]
    pieces = [(s, min(KCH, PTS - s)) for s in range(0, PTS, KCH)]
    load_k = [pltpu.make_async_copy(kmat.at[pl.ds(s, n)], kst.at[i % 2, pl.ds(0, n)], local_sem.at[4 + i])
              for i, (s, n) in enumerate(pieces)]
    start(load_c, load_o)

    plane = z * 8 + x * 2 + c

    def plane_dev(r):
        q = (plane + r) % 32
        return at(q // 8, (q // 2) % 4, q % 2, y)

    barrier = pltpu.get_barrier_semaphore()
    for dev in (up, down):
        pl.semaphore_signal(barrier, inc=1, device_id=dev, device_id_type=MESH)

    def greet(r, carry):
        pl.semaphore_signal(barrier, inc=1, device_id=plane_dev(r), device_id_type=MESH)
        return carry

    lax.fori_loop(1, 32, greet, 0)
    cbuf[g, :, pl.ds(PAD - 128, 128)] = jnp.zeros((DEEP_PAD, 128), BF16)
    cbuf[g, pl.ds(DEEP_PAD - 16, 16), :] = jnp.zeros((16, PAD), BF16)
    load_c.wait()
    cbuf[g, pl.ds(0, DEEP), pl.ds(0, PTS)] = cin[...]
    start(*load_g)
    load_o.wait()
    otown[:, pl.ds(PAD - 128, 128)] = jnp.zeros((ELEC, 128), BF16)
    otown[:, pl.ds(0, PTS)] = oin[...]

    @pl.when(is_same)
    def _():
        for h in range(2):
            otbuf[0, :, lanes[h]] = otown[:, cols[h]]

    pl.semaphore_wait(barrier, 33)

    def slot(zlo, yy):
        return zlo * 4 + yy

    def c_flow(k, h, dev, first=0, count=DEEP_PAD):
        ref = cbuf.at[k, pl.ds(first, count), cols[h]]
        return flow(ref, ref, dev)

    own_k, mate_k = slot(zl, y), slot(1 - zl, y)
    dn, un, on = (y + 3) % 4, (y + 1) % 4, (y + 2) % 4
    c_z, c_own, c_mate, c_far, c_zfar = [], [], [], [], []
    for h in range(2):
        c_z.append(c_flow(own_k, h, zmate))
        c_own.append((c_flow(own_k, h, up), c_flow(own_k, h, down)))
        c_mate.append((c_flow(mate_k, h, up), c_flow(mate_k, h, down)))
        c_far.append((c_flow(slot(zl, dn), h, up, 0, C_CUT),
                      c_flow(slot(zl, un), h, down, C_CUT, DEEP_PAD - C_CUT)))
        c_zfar.append(c_flow(slot(zl, on), h, zmate))
    start(*c_own[0], c_z[0], *c_own[1], c_z[1])

    def o_block(i, h):
        return otbuf.at[i, :, lanes[h]]

    o_xx = [flow(otown.at[:, cols[h]], o_block(0, h), xmate) for h in range(2)]
    o_right = [flow(o_block(0, h), o_block(1, h), right) for h in range(2)]
    o_left = [flow(o_block(0, h), o_block(2, h), left) for h in range(2)]
    o_sib = [flow(o_block(0, h), o_block(0, h), sib) for h in range(2)]
    o_far = [flow(o_block(1, 0), o_block(3, 0), right), flow(o_block(2, 1), o_block(3, 1), left)]
    o_relay = [[flow(o_block(i, h), o_block(i, h), sib) for h in range(2)] for i in (1, 2, 3)]
    o_first = [o_right[0], o_left[0], o_right[1], o_left[1]] + o_sib

    @pl.when(is_cross)
    def _():
        start(*o_xx)

    @pl.when(is_same)
    def _():
        start(*o_first)

    for cp in load_g:
        cp.wait()
    start(load_k[0], load_k[1])

    def cut_green(r, carry):
        rows = pl.ds(pl.multiple_of(r * 80, 16), 80)
        piece = gv[rows, :]
        for k in range(GROUPS):
            part = piece[:, k * DEEP:(k + 1) * DEEP]
            g8[k, rows, pl.ds(0, DEEP_PAD)] = jnp.concatenate([part, jnp.zeros((80, DEEP_PAD - DEEP), BF16)], axis=1)
        return carry

    lax.fori_loop(0, 10, cut_green, 0)

    def add_theta(k, h, first=False):
        part = dot(g8[k, :, pl.ds(0, DEEP_PAD)], cbuf[k, :, cols[h]])
        if first:
            acc[:, cols[h]] = part
        else:
            acc[:, cols[h]] += part

    def cut_kernel(i):
        s, n = pieces[i]
        load_k[i].wait()

        def rows_at(r, carry):
            rows = pl.ds(pl.multiple_of(r * 16, 16), 16)
            out = pl.ds(pl.multiple_of(s + r * 16, 16), 16)
            for b in range(16):
                j, core = b // 2, b % 2
                kb[j, out, pl.ds(core * 256, 256)] = kst[i % 2, rows, pl.ds(b * PTS, 256)]
                part = kst[i % 2, rows, pl.ds(b * PTS + 256, PTS - 256)]
                kb[j, out, pl.ds(512 + core * 384, 384)] = jnp.concatenate(
                    [part, jnp.zeros((16, PAD - PTS), BF16)], axis=1)
            return carry

        lax.fori_loop(0, (n + 15) // 16, rows_at, 0)
        if i + 2 < len(pieces):
            load_k[i + 2].start()

    def take(pair):
        for cp in pair:
            cp.wait_recv()

    def near_arrives(h):
        c_own[h][0].wait_recv()
        c_far[h][0].start()
        c_own[h][1].wait_recv()
        c_far[h][1].start()
        c_z[h].wait_recv()
        start(*c_mate[h])

    def far_arrives(h):
        take(c_far[h])
        c_zfar[h].start()

    add_theta(own_k, 0, True)
    cut_kernel(0)
    near_arrives(0)

    @pl.when(is_cross)
    def _():
        o_xx[0].wait_recv()
        start(o_right[0], o_left[0], o_sib[0])

    add_theta(own_k, 1, True)
    cut_kernel(1)
    near_arrives(1)

    @pl.when(is_cross)
    def _():
        o_xx[1].wait_recv()
        start(o_right[1], o_left[1], o_sib[1])

    def occupied_goes_on():
        for h in range(2):
            o_right[h].wait_recv()
            o_left[h].wait_recv()
        start(*o_far, *o_relay[0], *o_relay[1])

    add_theta(slot(zl, dn), 0)
    add_theta(slot(zl, un), 0)
    far_arrives(0)
    pl.when(is_same)(occupied_goes_on)
    add_theta(mate_k, 0)
    add_theta(slot(zl, on), 0)
    cut_kernel(2)
    take(c_mate[0])
    add_theta(slot(1 - zl, dn), 0)
    add_theta(slot(1 - zl, un), 0)

    far_arrives(1)
    c_zfar[0].wait_recv()
    add_theta(slot(1 - zl, on), 0)

    def t_block(i, h):
        return ttbuf.at[i, :, lanes[h]]

    def t_flows(count, make):
        return [[make(w, h) for h in range(2)] for w in range(count)]

    t_z = t_flows(2, lambda w, h: flow(ttown.at[w, :, cols[h]], t_block(2 + w, h), zmate))
    t_xx = t_flows(2, lambda w, h: flow(ttown.at[w, :, cols[h]], t_block(w, h), xmate))
    t_sib = t_flows(2, lambda w, h: flow(t_block(w, h), t_block(w, h), sib))
    t_sibz = t_flows(2, lambda w, h: flow(t_block(2 + w, h), t_block(2 + w, h), sib))
    t_right = t_flows(2, lambda w, h: flow(t_block(w * (1 + same), h), t_block(4 + w, h), right))
    t_left = t_flows(2, lambda w, h: flow(t_block(same + w * (1 + same), h), t_block(6 + w, h), left))
    low_r = (x + 1) % 4 < 2
    low_l = (x + 3) % 4 < 2
    go_r = 4 + jnp.where(is_same & jnp.logical_not(low_r), 1, 0)
    go_l = 6 + jnp.where(is_same & low_l, 0, 1)
    t_far = [[flow(t_block(go_r, h), t_block(8, h), right) for h in range(2)],
             [flow(t_block(go_l, h), t_block(9, h), left) for h in range(2)]]
    t_relay = [[flow(t_block(i, h), t_block(i, h), sib) for h in range(2)] for i in range(4, 10)]

    def publish(h):
        for w in range(2):
            t = acc[pl.ds(w * ELEC, ELEC), cols[h]].astype(BF16)
            ttown[w, :, cols[h]] = t

            @pl.when(is_same)
            def _():
                ttbuf[w, :, lanes[h]] = t

            dens[pl.ds(w, 1), cols[h]] = jnp.sum(
                t.astype(F32) * otown[:, cols[h]].astype(F32), axis=0, keepdims=True)

        @pl.when(is_cross)
        def _():
            start(t_xx[0][h], t_z[0][h], t_xx[1][h], t_z[1][h])

        @pl.when(is_same)
        def _():
            start(t_z[0][h], t_right[0][h], t_left[0][h], t_z[1][h], t_sib[0][h], t_sib[1][h])

    publish(0)
    pl.when(is_cross)(occupied_goes_on)
    for k in (mate_k, slot(zl, dn), slot(zl, un), slot(zl, on)):
        add_theta(k, 1)
    trans[...] = jnp.zeros_like(trans)
    take(c_mate[1])
    add_theta(slot(1 - zl, dn), 1)
    add_theta(slot(1 - zl, un), 1)
    c_zfar[1].wait_recv()
    add_theta(slot(1 - zl, on), 1)
    publish(1)

    dbuf[a] = dens[...].astype(BF16).astype(F32)

    def d_flow(r):
        return pltpu.make_async_remote_copy(
            src_ref=dbuf.at[a], dst_ref=dbuf.at[a], send_sem=d_send.at[r], recv_sem=d_recv.at[r],
            device_id={"pts": (a + r) % 16, "wlk": g}, device_id_type=MESH)

    def d_start(r, carry):
        d_flow(r).start()
        return carry

    def d_wait(r, carry):
        d_flow(r).wait()
        return carry

    lax.fori_loop(1, 16, d_start, 0)
    cut_kernel(3)
    kb[:, pl.ds(PTS, ROWS - PTS), :] = jnp.zeros((8, ROWS - PTS, 2 * PAD), BF16)

    def turned(src, size):
        trans[pl.ds(0, ELEC), pl.ds(0, size)] = src.astype(F32)
        return jnp.swapaxes(trans[:, pl.ds(0, size)], 0, 1).astype(BF16)

    def turn(side, h):
        tp[side, cols[h], :] = turned(ttbuf[side, :, lanes[h]], CHUNK[h][1])

    def potential():
        pot[...] = jnp.zeros_like(pot)

        def add_chip(j, carry):
            one, two = dbuf[2 * j].astype(BF16), dbuf[2 * j + 1].astype(BF16)
            both = jnp.concatenate([one[:, :256], two[:, :256], one[:, 256:], two[:, 256:]], axis=1)
            pot[...] += lax.dot_general(both, kb[j], (((1,), (1,)), ((), ())), preferred_element_type=F32)
            return carry

        lax.fori_loop(0, 8, add_chip, 0)
        pot_out[...] = pot[:, pl.ds(0, PTS)]

    exch[...] = jnp.zeros_like(exch)

    def unit(tt, side, ot, chip, weight, h):
        left_t = tp[side, pl.ds(0, ROWS), pl.ds(0, ELEC)]
        left_o = op[pl.ds(0, ROWS), pl.ds(0, ELEC)]

        def step(n, carry):
            part = pl.ds(n * 256, 256)
            near = dot(left_t, otbuf[ot, :, part])
            away = dot(left_o, ttbuf[tt, :, part])
            terms = kb[chip, :, part].astype(F32) * near * away
            return carry + terms.reshape(ROWS // 8, 8, 256).sum(axis=0)

        total = jnp.zeros((8, 256), F32)
        for n in range(*STEPS[h]):
            total = step(n, total)
        exch[side] += weight * total

    far_zh = jnp.where(is_same, zh, 1 - zh) * 4
    chip_0, chip_1, chip_2, chip_3 = (far_zh + (x + d) % 4 for d in (0, 3, 1, 2))
    cross2 = 2 * (1 - same)
    self_weight = jnp.where(is_same, 1.0, 2.0)
    far_side = jnp.where(is_cross | (x >= 2), 2, 0)
    units = {
        0: (cross2, 0, chip_0, self_weight), 1: (cross2 + 1, 0, chip_0, self_weight),
        2: (2, 0, chip_0, self_weight), 3: (3, 0, chip_0, self_weight),
        4: (cross2, 1, chip_1, 2.0), 5: (3 - same, 1, chip_1, 2.0),
        6: (cross2 + same, 2, chip_2, 2.0), 7: (3, 2, chip_2, 2.0),
        8: (far_side, 3, chip_3, 2.0), 9: (far_side + 1, 3, chip_3, 2.0),
    }

    def run(tt, h):
        unit(tt, *units[tt], h)

    def pass_same(w, h):
        t_z[w][h].wait_recv()
        start(t_right[1][h] if w == 0 else t_left[1][h], t_sibz[w][h])
        turn(2 + w, h)

    def pass_cross(w, h):
        t_xx[w][h].wait_recv()
        start(t_right[w][h], t_left[w][h], t_sib[w][h])
        t_z[w][h].wait_recv()
        turn(2 + w, h)

    def from_left(w, h):
        t_right[w][h].wait_recv()
        t_relay[w][h].start()

    def from_right(w, h):
        t_left[w][h].wait_recv()
        t_relay[2 + w][h].start()

    def from_far(w, h):
        t_far[w][h].wait_recv()
        t_relay[4 + w][h].start()

    def relayed(tt, h):
        t_relay[tt - 4][h].wait_recv()
        run(tt, h)

    op[...] = turned(otown[...], PAD)

    @pl.when(is_same)
    def _():
        for w in range(2):
            for h in range(2):
                turn(w, h)
        take(o_sib)
        take(t_sib[0])
        run(0, 0)
        pass_same(0, 0)
        from_left(0, 0)
        from_right(0, 0)
        run(0, 1)
        take(t_sib[1])
        run(1, 0)
        pass_same(1, 0)
        run(1, 1)
        take(o_far)
        start(*o_relay[2])
        from_left(0, 1)
        from_right(0, 1)
        take(o_relay[0])
        take(o_relay[1])
        relayed(4, 0)
        relayed(6, 0)
        pass_same(0, 1)
        from_left(1, 0)
        from_right(1, 0)
        start(t_far[0][0], t_far[1][0])
        relayed(4, 1)
        relayed(6, 1)
        take(t_sibz[0])
        run(2, 0)
        run(2, 1)
        pass_same(1, 1)
        relayed(5, 0)
        relayed(7, 0)
        from_left(1, 1)
        t_far[0][1].start()
        take(t_sibz[1])
        run(3, 0)
        run(3, 1)
        relayed(5, 1)
        from_far(0, 0)
        from_far(1, 0)
        from_right(1, 1)
        t_far[1][1].start()
        lax.fori_loop(1, 16, d_wait, 0)
        potential()
        relayed(7, 1)
        take(o_relay[2])
        relayed(8, 0)
        relayed(9, 0)
        from_far(0, 1)
        relayed(8, 1)
        from_far(1, 1)
        relayed(9, 1)

    @pl.when(is_cross)
    def _():
        pass_cross(0, 0)
        take(o_far)
        start(*o_relay[2])
        pass_cross(1, 0)
        from_left(0, 0)
        from_right(0, 0)
        t_far[0][0].start()
        pass_cross(0, 1)
        take(o_sib)
        take(t_sib[0])
        run(0, 0)
        run(0, 1)
        from_left(1, 0)
        from_right(1, 0)
        t_far[1][0].start()
        take(o_relay[0])
        take(o_relay[1])
        relayed(4, 0)
        relayed(6, 0)
        pass_cross(1, 1)
        take(t_sib[1])
        run(1, 0)
        run(1, 1)
        relayed(5, 0)
        relayed(7, 0)
        from_left(0, 1)
        from_right(0, 1)
        t_far[0][1].start()
        from_far(0, 0)
        from_far(1, 0)
        relayed(4, 1)
        relayed(6, 1)
        take(o_relay[2])
        from_left(1, 1)
        from_right(1, 1)
        t_far[1][1].start()
        relayed(8, 0)
        relayed(9, 0)
        relayed(5, 1)
        relayed(7, 1)
        lax.fori_loop(1, 16, d_wait, 0)
        potential()
        from_far(0, 1)
        relayed(8, 1)
        from_far(1, 1)
        relayed(9, 1)

    row = lax.broadcasted_iota(jnp.int32, (8, 128), 0)
    tile = jnp.zeros((8, 128), F32)
    for side in range(4):
        tile = jnp.where(row == (zl * 2 + side) % 4, -0.5 * jnp.sum(exch[side]), tile)
    for w in range(2):
        tile = jnp.where(row == 4 + zl * 2 + w,
                         0.5 * jnp.sum(dens[pl.ds(w, 1), pl.ds(0, PTS)] * pot[pl.ds(w, 1), pl.ds(0, PTS)]), tile)
    ebuf[plane] = tile

    def e_flow(r):
        return pltpu.make_async_remote_copy(
            src_ref=ebuf.at[plane], dst_ref=ebuf.at[plane], send_sem=e_send.at[r], recv_sem=e_recv.at[r],
            device_id=plane_dev(r), device_id_type=MESH)

    def e_start(r, carry):
        e_flow(r).start()
        return carry

    def e_wait(r, carry):
        e_flow(r).wait()
        return carry

    lax.fori_loop(1, 32, e_start, 0)

    for pairs in (c_own, c_mate, c_far, t_z, t_right, t_left, t_sib, t_far, t_relay, o_relay):
        for pair in pairs:
            for cp in pair:
                cp.wait_send()
    for cp in c_z + c_zfar + o_first + o_far:
        cp.wait_send()

    @pl.when(is_cross)
    def _():
        for cp in o_xx + t_xx[0] + t_xx[1]:
            cp.wait_send()

    @pl.when(is_same)
    def _():
        for cp in t_sibz[0] + t_sibz[1]:
            cp.wait_send()

    lax.fori_loop(1, 32, e_wait, 0)
    sum_out[...] = ebuf[...].sum(axis=0)


def finish(pot, total, pot_out, cou_out, exc_out):
    zl = lax.axis_index("wlk") // 4
    pot_out[...] = pot[...]
    row = lax.broadcasted_iota(jnp.int32, (8, 128), 0)
    for w in range(2):
        exc_out[w] = jnp.sum(jnp.where(row == zl * 2 + w, total[...], 0.0)) * (1.0 / 128)
        cou_out[w] = jnp.sum(jnp.where(row == 4 + zl * 2 + w, total[...], 0.0)) * (1.0 / 128)


def local(green_half, collocation, occupied, kernel):
    any_space = pl.BlockSpec(memory_space=pl.ANY)
    vmem = pltpu.VMEM
    in_vmem, in_smem = pl.BlockSpec(memory_space=vmem), pl.BlockSpec(memory_space=pltpu.SMEM)
    pot, total = pl.pallas_call(
        body,
        out_shape=(jax.ShapeDtypeStruct((2, PTS), F32), jax.ShapeDtypeStruct((8, 128), F32)),
        in_specs=[any_space] * 4,
        out_specs=(in_vmem, in_vmem),
        scratch_shapes=[
            vmem((DEEP, PTS), BF16),
            vmem((ELEC, PTS), BF16),
            vmem((2 * ELEC, 8 * DEEP), BF16),
            vmem((GROUPS, 2 * ELEC, 384), BF16),
            vmem((2, KCH, 16 * PTS), BF16),
            vmem((8, ROWS, 2 * PAD), BF16),
            vmem((GROUPS, DEEP_PAD, PAD), BF16),
            vmem((2 * ELEC, PAD), F32),
            vmem((2, ELEC, PAD), BF16),
            vmem((10, ELEC, 2 * PAD), BF16),
            vmem((4, PAD, 512), BF16),
            vmem((PAD, 512), BF16),
            vmem((ELEC, PAD), BF16),
            vmem((4, ELEC, 2 * PAD), BF16),
            vmem((512, PAD), F32),
            vmem((2, PAD), F32),
            vmem((16, 2, PAD), F32),
            vmem((32, 8, 128), F32),
            vmem((4, 8, 256), F32),
            vmem((2, ROWS), F32),
            pltpu.SemaphoreType.DMA((8,)),
            pltpu.SemaphoreType.DMA((FLOWS,)),
            pltpu.SemaphoreType.DMA((FLOWS,)),
            pltpu.SemaphoreType.DMA((16,)),
            pltpu.SemaphoreType.DMA((16,)),
            pltpu.SemaphoreType.DMA((32,)),
            pltpu.SemaphoreType.DMA((32,)),
        ],
        compiler_params=pltpu.CompilerParams(
            collective_id=0, has_side_effects=True, vmem_limit_bytes=67_000_000),
    )(green_half, collocation, occupied.T, kernel)
    return pl.pallas_call(
        finish,
        out_shape=(jax.ShapeDtypeStruct((2, PTS), F32), jax.ShapeDtypeStruct((2,), F32), jax.ShapeDtypeStruct((2,), F32)),
        in_specs=[in_vmem, in_vmem],
        out_specs=(in_vmem, in_smem, in_smem),
    )(pot, total)


def solution(mesh):
    placed = (P("wlk", None, None), P("wlk", "pts"), P("pts", None), P("pts", None))
    return jax.shard_map(
        local,
        mesh=mesh,
        in_specs=placed,
        out_specs=(P("wlk", "pts"), P("wlk"), P("wlk")),
        check_vma=False,
    )
```

```python
import jax
import jax.numpy as jnp
from jax import lax
from jax.experimental import pallas as pl
from jax.experimental.pallas import tpu as pltpu
from jax.sharding import PartitionSpec as P

MESH = pl.DeviceIdType.MESH
F32, BF16 = jnp.float32, jnp.bfloat16

ELEC = 400
PTS = 600
PAD = 640
ROWS = 608
DEEP = 300
DEEP_PAD = 304
GROUPS = 8
C_CUT = 160
KCH = 160
CHUNK = ((0, 256), (256, 256), (512, 128))
PARTS = range(len(CHUNK))
STEPS = ((0, 2), (2, 4), (4, 5))
FLOWS = 144


def dot(a, b):
    return jnp.dot(a, b, preferred_element_type=F32)


def body(green, colloc, occ, kmat, pot_out, sum_out,
         cin, oin, gv, g8, kst, kb, cbuf, acc, ttown, ttbuf, tp, op, otown, otbuf,
         trans, dens, dbuf, ebuf, exch, pot, local_sem, send, recv, d_send, d_recv, e_send, e_recv, hear):
    a, g = lax.axis_index("pts"), lax.axis_index("wlk")
    zh, x, c = a // 8, (a // 2) % 4, a % 2
    zl, y = g // 4, g % 4
    z = zh * 2 + zl
    is_same = zh == zl
    is_cross = zh != zl
    same = is_same.astype(jnp.int32)

    def at(zz, xx, cc, yy):
        return {"pts": (zz // 2) * 8 + xx * 2 + cc, "wlk": (zz % 2) * 4 + yy}

    sib = at(z, x, 1 - c, y)
    right, left = at(z, (x + 1) % 4, c, y), at(z, (x + 3) % 4, c, y)
    up, down = at(z, x, c, (y + 1) % 4), at(z, x, c, (y + 3) % 4)
    zmate = at(zh * 2 + 1 - zl, x, c, y)
    xmate = at(3 - z, x, c, y)
    lanes = tuple(pl.ds(pl.multiple_of(2 * start + c * size, 128), size) for start, size in CHUNK)
    cols = tuple(pl.ds(start, size) for start, size in CHUNK)
    numbers = iter(range(FLOWS))

    def flow(src, dst, dev):
        f = next(numbers)
        return pltpu.make_async_remote_copy(
            src_ref=src, dst_ref=dst, send_sem=send.at[f], recv_sem=recv.at[f],
            device_id=dev, device_id_type=MESH)

    def start(*copies):
        for cp in copies:
            cp.start()

    load_c = pltpu.make_async_copy(colloc, cin, local_sem.at[0])
    load_o = pltpu.make_async_copy(occ, oin, local_sem.at[1])
    load_g = [pltpu.make_async_copy(green.at[w], gv.at[pl.ds(w * ELEC, ELEC)], local_sem.at[2 + w]) for w in range(2)]
    pieces = [(s, min(KCH, PTS - s)) for s in range(0, PTS, KCH)]
    load_k = [pltpu.make_async_copy(kmat.at[pl.ds(s, n)], kst.at[i % 2, pl.ds(0, n)], local_sem.at[4 + i])
              for i, (s, n) in enumerate(pieces)]
    start(load_c, load_o)

    plane = z * 8 + x * 2 + c

    def plane_dev(r):
        q = (plane + r) % 32
        return at(q // 8, (q // 2) % 4, q % 2, y)

    barrier = pltpu.get_barrier_semaphore()
    for dev in (up, down, right, left, zmate, xmate, sib):
        pl.semaphore_signal(barrier, inc=1, device_id=dev, device_id_type=MESH)

    rounds = ((right, left), (right, left), (zmate, xmate), (sib,))

    def tell(r):
        for dev in rounds[r]:
            pl.semaphore_signal(hear.at[r], inc=1, device_id=dev, device_id_type=MESH)

    def heard(r):
        pl.semaphore_wait(hear.at[r], len(rounds[r]))
        if r + 1 < len(rounds):
            tell(r + 1)
    cbuf[g, :, pl.ds(PAD - 128, 128)] = jnp.zeros((DEEP_PAD, 128), BF16)
    cbuf[g, pl.ds(DEEP_PAD - 16, 16), :] = jnp.zeros((16, PAD), BF16)
    load_c.wait()
    cbuf[g, pl.ds(0, DEEP), pl.ds(0, PTS)] = cin[...]
    start(*load_g)
    load_o.wait()
    otown[:, pl.ds(PAD - 128, 128)] = jnp.zeros((ELEC, 128), BF16)
    otown[:, pl.ds(0, PTS)] = oin[...]

    @pl.when(is_same)
    def _():
        for h in PARTS:
            otbuf[0, :, lanes[h]] = otown[:, cols[h]]

    pl.semaphore_wait(barrier, 7)
    tell(0)

    def slot(zlo, yy):
        return zlo * 4 + yy

    def c_flow(k, h, dev, first=0, count=DEEP_PAD):
        ref = cbuf.at[k, pl.ds(first, count), cols[h]]
        return flow(ref, ref, dev)

    own_k, mate_k = slot(zl, y), slot(1 - zl, y)
    dn, un, on = (y + 3) % 4, (y + 1) % 4, (y + 2) % 4
    c_z, c_own, c_mate, c_far, c_zfar = [], [], [], [], []
    for h in PARTS:
        c_z.append(c_flow(own_k, h, zmate))
        c_own.append((c_flow(own_k, h, up), c_flow(own_k, h, down)))
        c_mate.append((c_flow(mate_k, h, up), c_flow(mate_k, h, down)))
        c_far.append((c_flow(slot(zl, dn), h, up, 0, C_CUT),
                      c_flow(slot(zl, un), h, down, C_CUT, DEEP_PAD - C_CUT)))
        c_zfar.append(c_flow(slot(zl, on), h, zmate))
    for h in PARTS:
        start(*c_own[h], c_z[h])

    def o_block(i, h):
        return otbuf.at[i, :, lanes[h]]

    o_xx = [flow(otown.at[:, cols[h]], o_block(0, h), xmate) for h in PARTS]
    o_right = [flow(o_block(0, h), o_block(1, h), right) for h in PARTS]
    o_left = [flow(o_block(0, h), o_block(2, h), left) for h in PARTS]
    o_sib = [flow(o_block(0, h), o_block(0, h), sib) for h in PARTS]
    o_far = [flow(o_block(1, 0), o_block(3, 0), right), flow(o_block(2, 1), o_block(3, 1), left),
             flow(o_block(1, 2), o_block(3, 2), right)]
    o_relay = [[flow(o_block(i, h), o_block(i, h), sib) for h in PARTS] for i in (1, 2, 3)]
    o_first = o_right + o_left + o_sib

    @pl.when(is_cross)
    def _():
        start(*o_xx)

    @pl.when(is_same)
    def _():
        for h in PARTS:
            start(o_right[h], o_left[h], o_sib[h])

    for cp in load_g:
        cp.wait()
    start(load_k[0], load_k[1])

    def cut_green(r, carry):
        rows = pl.ds(pl.multiple_of(r * 80, 16), 80)
        piece = gv[rows, :]
        for k in range(GROUPS):
            part = piece[:, k * DEEP:(k + 1) * DEEP]
            g8[k, rows, pl.ds(0, DEEP_PAD)] = jnp.concatenate([part, jnp.zeros((80, DEEP_PAD - DEEP), BF16)], axis=1)
        return carry

    lax.fori_loop(0, 10, cut_green, 0)
    heard(0)

    def add_theta(k, h, first=False):
        part = dot(g8[k, :, pl.ds(0, DEEP_PAD)], cbuf[k, :, cols[h]])
        if first:
            acc[:, cols[h]] = part
        else:
            acc[:, cols[h]] += part

    def cut_kernel(i):
        s, n = pieces[i]
        load_k[i].wait()

        def rows_at(r, carry):
            rows = pl.ds(pl.multiple_of(r * 16, 16), 16)
            out = pl.ds(pl.multiple_of(s + r * 16, 16), 16)
            for b in range(16):
                j, core = b // 2, b % 2
                kb[j, out, pl.ds(core * 256, 256)] = kst[i % 2, rows, pl.ds(b * PTS, 256)]
                kb[j, out, pl.ds(512 + core * 256, 256)] = kst[i % 2, rows, pl.ds(b * PTS + 256, 256)]
                part = kst[i % 2, rows, pl.ds(b * PTS + 512, PTS - 512)]
                kb[j, out, pl.ds(1024 + core * 128, 128)] = jnp.concatenate(
                    [part, jnp.zeros((16, PAD - PTS), BF16)], axis=1)
            return carry

        lax.fori_loop(0, (n + 15) // 16, rows_at, 0)
        if i + 2 < len(pieces):
            load_k[i + 2].start()

    def take(pair):
        for cp in pair:
            cp.wait_recv()

    def near_arrives(h):
        c_own[h][0].wait_recv()
        c_far[h][0].start()
        c_own[h][1].wait_recv()
        c_far[h][1].start()
        c_z[h].wait_recv()
        start(*c_mate[h])

    def far_arrives(h):
        take(c_far[h])
        c_zfar[h].start()

    for h in PARTS:
        add_theta(own_k, h, True)
    cut_kernel(0)
    heard(1)
    near_arrives(0)

    @pl.when(is_cross)
    def _():
        o_xx[0].wait_recv()
        start(o_right[0], o_left[0], o_sib[0])

    cut_kernel(1)
    near_arrives(1)
    near_arrives(2)
    heard(2)

    @pl.when(is_cross)
    def _():
        for h in (1, 2):
            o_xx[h].wait_recv()
            start(o_right[h], o_left[h], o_sib[h])

    def occupied_part(h):
        o_right[h].wait_recv()
        o_left[h].wait_recv()
        start(o_far[h], o_relay[0][h], o_relay[1][h])

    def occupied_goes_on():
        for h in PARTS:
            occupied_part(h)

    def add_near(h):
        add_theta(slot(zl, dn), h)
        add_theta(slot(zl, un), h)
        add_theta(mate_k, h)

    def add_mates(h):
        take(c_mate[h])
        add_theta(slot(1 - zl, dn), h)
        add_theta(slot(1 - zl, un), h)

    add_near(0)
    far_arrives(0)
    pl.when(is_same)(occupied_goes_on)

    @pl.when(is_cross)
    def _():
        occupied_part(0)

    add_theta(slot(zl, on), 0)
    add_near(1)
    add_mates(0)
    far_arrives(1)

    @pl.when(is_cross)
    def _():
        occupied_part(1)

    c_zfar[0].wait_recv()
    add_theta(slot(1 - zl, on), 0)

    def t_block(i, h):
        return ttbuf.at[i, :, lanes[h]]

    def t_flows(count, make):
        return [[make(w, h) for h in PARTS] for w in range(count)]

    t_z = t_flows(2, lambda w, h: flow(ttown.at[w, :, cols[h]], t_block(2 + w, h), zmate))
    t_xx = t_flows(2, lambda w, h: flow(ttown.at[w, :, cols[h]], t_block(w, h), xmate))
    t_sib = t_flows(2, lambda w, h: flow(t_block(w, h), t_block(w, h), sib))
    t_sibz = t_flows(2, lambda w, h: flow(t_block(2 + w, h), t_block(2 + w, h), sib))
    t_right = t_flows(2, lambda w, h: flow(t_block(w * (1 + same), h), t_block(4 + w, h), right))
    t_left = t_flows(2, lambda w, h: flow(t_block(same + w * (1 + same), h), t_block(6 + w, h), left))
    low_r = (x + 1) % 4 < 2
    low_l = (x + 3) % 4 < 2
    go_r = 4 + jnp.where(is_same & jnp.logical_not(low_r), 1, 0)
    go_l = 6 + jnp.where(is_same & low_l, 0, 1)
    t_far = [[flow(t_block(go_r, h), t_block(8, h), right) for h in PARTS],
             [flow(t_block(go_l, h), t_block(9, h), left) for h in PARTS]]
    t_relay = [[flow(t_block(i, h), t_block(i, h), sib) for h in PARTS] for i in range(4, 10)]

    def publish(h):
        for w in range(2):
            t = acc[pl.ds(w * ELEC, ELEC), cols[h]].astype(BF16)
            ttown[w, :, cols[h]] = t

            @pl.when(is_same)
            def _():
                ttbuf[w, :, lanes[h]] = t

            dens[pl.ds(w, 1), cols[h]] = jnp.sum(
                t.astype(F32) * otown[:, cols[h]].astype(F32), axis=0, keepdims=True)

        @pl.when(is_same)
        def _():
            start(t_right[0][h], t_left[0][h], t_sib[0][h], t_sib[1][h])

    publish(0)
    heard(3)

    @pl.when(is_cross)
    def _():
        start(t_xx[0][0], t_xx[1][0])

    add_theta(slot(zl, on), 1)
    add_near(2)
    far_arrives(2)
    start(t_z[0][0])

    @pl.when(is_cross)
    def _():
        start(t_z[1][0])

    @pl.when(is_cross)
    def _():
        occupied_part(2)

    add_mates(1)
    c_zfar[1].wait_recv()
    add_theta(slot(1 - zl, on), 1)
    publish(1)

    add_theta(slot(zl, on), 2)
    add_mates(2)
    c_zfar[2].wait_recv()
    add_theta(slot(1 - zl, on), 2)
    publish(2)

    dbuf[a] = dens[...].astype(BF16).astype(F32)

    def d_flow(r):
        return pltpu.make_async_remote_copy(
            src_ref=dbuf.at[a], dst_ref=dbuf.at[a], send_sem=d_send.at[r], recv_sem=d_recv.at[r],
            device_id={"pts": (a + r) % 16, "wlk": g}, device_id_type=MESH)

    def d_start(r, carry):
        d_flow(r).start()
        return carry

    def d_wait(r, carry):
        d_flow(r).wait()
        return carry

    lax.fori_loop(1, 16, d_start, 0)

    @pl.when(is_cross)
    def _():
        start(t_xx[0][1], t_xx[1][1], t_xx[0][2], t_xx[1][2], t_z[0][1], t_z[1][1], t_z[0][2], t_z[1][2])

    @pl.when(is_same)
    def _():
        start(t_z[0][1], t_z[0][2], *t_z[1])

    def turned(src, size):
        trans[pl.ds(0, ELEC), pl.ds(0, size)] = src.astype(F32)
        return jnp.swapaxes(trans[:, pl.ds(0, size)], 0, 1).astype(BF16)

    def turn(side, h):
        tp[side, cols[h], :] = turned(ttbuf[side, :, lanes[h]], CHUNK[h][1])

    def potential(first):
        if first == 0:
            pot[...] = jnp.zeros_like(pot)

        def add_chip(j, carry):
            one, two = dbuf[2 * j].astype(BF16), dbuf[2 * j + 1].astype(BF16)
            both = jnp.concatenate([v[:, i:i + n] for i, n in CHUNK for v in (one, two)], axis=1)
            pot[...] += lax.dot_general(both, kb[j], (((1,), (1,)), ((), ())), preferred_element_type=F32)
            return carry

        lax.fori_loop(first, first + 4, add_chip, 0)
        if first:
            pot_out[...] = pot[:, pl.ds(0, PTS)]

    exch[...] = jnp.zeros_like(exch)

    def unit(tt, side, ot, chip, weight, h):
        left_t = tp[side, pl.ds(0, ROWS), pl.ds(0, ELEC)]
        left_o = op[pl.ds(0, ROWS), pl.ds(0, ELEC)]

        def step(n, carry):
            part = pl.ds(n * 256, 256)
            near = dot(left_t, otbuf[ot, :, part])
            away = dot(left_o, ttbuf[tt, :, part])
            terms = kb[chip, :, part].astype(F32) * near * away
            return carry + terms.reshape(ROWS // 8, 8, 256).sum(axis=0)

        total = jnp.zeros((8, 256), F32)
        for n in range(*STEPS[h]):
            total = step(n, total)
        exch[side] += weight * total

    def cross_go(w, h):
        t_xx[w][h].wait_recv()
        start(t_right[w][h], t_left[w][h], t_sib[w][h])

    def z_take(w, h):
        t_z[w][h].wait_recv()
        turn(2 + w, h)

    def same_go(w, h):
        t_z[w][h].wait_recv()
        start(t_right[1][h] if w == 0 else t_left[1][h], t_sibz[w][h])
        turn(2 + w, h)

    def from_left(w, h):
        t_right[w][h].wait_recv()
        t_relay[w][h].start()

    def from_right(w, h):
        t_left[w][h].wait_recv()
        t_relay[2 + w][h].start()

    def from_both(w, h):
        from_left(w, h)
        from_right(w, h)

    def from_far(w, h):
        t_far[w][h].wait_recv()
        t_relay[4 + w][h].start()

    base = jnp.where(is_same, zh, 1 - zh) * 4
    of_same = {0: (0, 0, 0, 1.0), 1: (1, 0, 0, 1.0), 2: (2, 0, 0, 1.0), 3: (3, 0, 0, 1.0),
               4: (0, 1, 3, 2.0), 5: (2, 1, 3, 2.0), 6: (1, 2, 1, 2.0), 7: (3, 2, 1, 2.0),
               8: (2 * (x // 2), 3, 2, 2.0), 9: (2 * (x // 2) + 1, 3, 2, 2.0)}
    of_cross = {0: (2, 0, 0, 2.0), 1: (3, 0, 0, 2.0), 4: (2, 1, 3, 2.0), 5: (3, 1, 3, 2.0),
                6: (2, 2, 1, 2.0), 7: (3, 2, 1, 2.0), 8: (2, 3, 2, 2.0), 9: (3, 3, 2, 2.0)}

    def handed(i, h):
        return t_sib[i][h] if i < 2 else t_sibz[i - 2][h] if i < 4 else t_relay[i - 4][h]

    def run(s_block, x_block, h):
        @pl.when(is_same)
        def _():
            handed(s_block, h).wait_recv()

        @pl.when(is_cross)
        def _():
            handed(x_block, h).wait_recv()

        picked = [jnp.where(is_same, u, v) for u, v in zip((s_block, *of_same[s_block]), (x_block, *of_cross[x_block]))]
        unit(picked[0], picked[1], picked[2], base + (x + picked[3]) % 4, picked[4], h)

    def own(i, h):
        handed(i, h).wait_recv()
        side, ot, away, weight = of_same[i]
        unit(i, side, ot, base + (x + away) % 4, weight, h)

    op[...] = turned(otown[...], PAD)

    @pl.when(is_cross)
    def _():
        cross_go(0, 0)

    cut_kernel(2)

    @pl.when(is_same)
    def _():
        same_go(0, 0)
        from_both(0, 0)

    @pl.when(is_cross)
    def _():
        cross_go(1, 0)

    cut_kernel(3)
    kb[:, pl.ds(PTS, ROWS - PTS), :] = jnp.zeros((8, ROWS - PTS, 2 * PAD), BF16)
    take(o_sib)

    @pl.when(is_same)
    def _():
        for w in range(2):
            for h in PARTS:
                turn(w, h)
        own(0, 0)
        own(0, 1)
        own(0, 2)
        same_go(1, 0)
        own(1, 0)
        own(1, 1)
        own(1, 2)
        from_both(0, 1)

    @pl.when(is_cross)
    def _():
        z_take(0, 0)

    take(o_far)
    start(*o_relay[2])
    lax.fori_loop(1, 16, d_wait, 0)
    potential(0)

    @pl.when(is_cross)
    def _():
        from_both(0, 0)
        z_take(0, 1)
        cross_go(0, 1)

    @pl.when(is_same)
    def _():
        from_both(0, 2)
        same_go(0, 1)

    potential(4)
    for part in o_relay:
        take(part)

    @pl.when(is_cross)
    def _():
        z_take(0, 2)
        from_both(1, 0)

    run(4, 0, 0)

    @pl.when(is_cross)
    def _():
        cross_go(1, 1)
        t_far[0][0].start()
        t_far[1][0].start()

    run(4, 0, 1)

    @pl.when(is_same)
    def _():
        from_left(1, 0)
        t_far[0][0].start()
        same_go(1, 1)

    run(6, 4, 0)

    @pl.when(is_cross)
    def _():
        cross_go(0, 2)

    run(2, 6, 0)

    @pl.when(is_same)
    def _():
        same_go(0, 2)
        from_right(1, 0)
        t_far[1][0].start()

    @pl.when(is_cross)
    def _():
        z_take(1, 0)

    run(4, 0, 2)

    @pl.when(is_cross)
    def _():
        cross_go(1, 2)
        from_both(0, 1)
        t_far[0][1].start()

    run(6, 4, 1)

    @pl.when(is_same)
    def _():
        same_go(1, 2)

    run(2, 6, 1)

    @pl.when(is_same)
    def _():
        from_left(1, 1)
        t_far[0][1].start()

    @pl.when(is_cross)
    def _():
        z_take(1, 1)
        z_take(1, 2)

    run(3, 1, 0)
    run(3, 1, 1)

    @pl.when(is_cross)
    def _():
        from_both(1, 1)
        t_far[1][1].start()

    run(5, 5, 0)

    @pl.when(is_same)
    def _():
        from_right(1, 1)
        t_far[1][1].start()

    run(7, 7, 0)
    run(6, 1, 2)
    from_far(0, 0)

    @pl.when(is_cross)
    def _():
        from_both(0, 2)
        t_far[0][2].start()

    @pl.when(is_same)
    def _():
        from_left(1, 2)
        t_far[0][2].start()

    run(5, 5, 1)
    run(8, 8, 0)
    from_far(1, 0)

    @pl.when(is_cross)
    def _():
        from_both(1, 2)
        t_far[1][2].start()

    @pl.when(is_same)
    def _():
        from_right(1, 2)
        t_far[1][2].start()

    run(7, 7, 1)
    run(9, 9, 0)
    run(2, 4, 2)
    run(3, 6, 2)
    run(5, 5, 2)
    from_far(0, 1)
    run(7, 7, 2)
    from_far(1, 1)
    run(8, 8, 1)
    from_far(0, 2)
    run(9, 9, 1)
    from_far(1, 2)
    run(8, 8, 2)
    run(9, 9, 2)

    row = lax.broadcasted_iota(jnp.int32, (8, 128), 0)
    tile = jnp.zeros((8, 128), F32)
    for side in range(4):
        tile = jnp.where(row == (zl * 2 + side) % 4, -0.5 * jnp.sum(exch[side]), tile)
    for w in range(2):
        tile = jnp.where(row == 4 + zl * 2 + w,
                         0.5 * jnp.sum(dens[pl.ds(w, 1), pl.ds(0, PTS)] * pot[pl.ds(w, 1), pl.ds(0, PTS)]), tile)
    ebuf[plane] = tile

    def e_flow(r):
        return pltpu.make_async_remote_copy(
            src_ref=ebuf.at[plane], dst_ref=ebuf.at[plane], send_sem=e_send.at[r], recv_sem=e_recv.at[r],
            device_id=plane_dev(r), device_id_type=MESH)

    def e_wait(r, carry):
        e_flow(r).wait()
        return carry

    for r in (*range(16, 32), *range(15, 0, -1)):
        e_flow(r).start()

    for pairs in (c_own, c_mate, c_far, t_z, t_right, t_left, t_sib, t_far, t_relay, o_relay):
        for pair in pairs:
            for cp in pair:
                cp.wait_send()
    for cp in c_z + c_zfar + o_first + o_far:
        cp.wait_send()

    @pl.when(is_cross)
    def _():
        for cp in o_xx + t_xx[0] + t_xx[1]:
            cp.wait_send()

    @pl.when(is_same)
    def _():
        for cp in t_sibz[0] + t_sibz[1]:
            cp.wait_send()

    lax.fori_loop(1, 32, e_wait, 0)
    sum_out[...] = ebuf[...].sum(axis=0)


def finish(pot, total, pot_out, cou_out, exc_out):
    zl = lax.axis_index("wlk") // 4
    pot_out[...] = pot[...]
    row = lax.broadcasted_iota(jnp.int32, (8, 128), 0)
    for w in range(2):
        exc_out[w] = jnp.sum(jnp.where(row == zl * 2 + w, total[...], 0.0)) * (1.0 / 128)
        cou_out[w] = jnp.sum(jnp.where(row == 4 + zl * 2 + w, total[...], 0.0)) * (1.0 / 128)


def local(green_half, collocation, occupied, kernel):
    any_space = pl.BlockSpec(memory_space=pl.ANY)
    vmem = pltpu.VMEM
    in_vmem, in_smem = pl.BlockSpec(memory_space=vmem), pl.BlockSpec(memory_space=pltpu.SMEM)
    pot, total = pl.pallas_call(
        body,
        out_shape=(jax.ShapeDtypeStruct((2, PTS), F32), jax.ShapeDtypeStruct((8, 128), F32)),
        in_specs=[any_space] * 4,
        out_specs=(in_vmem, in_vmem),
        scratch_shapes=[
            vmem((DEEP, PTS), BF16),
            vmem((ELEC, PTS), BF16),
            vmem((2 * ELEC, 8 * DEEP), BF16),
            vmem((GROUPS, 2 * ELEC, 384), BF16),
            vmem((2, KCH, 16 * PTS), BF16),
            vmem((8, ROWS, 2 * PAD), BF16),
            vmem((GROUPS, DEEP_PAD, PAD), BF16),
            vmem((2 * ELEC, PAD), F32),
            vmem((2, ELEC, PAD), BF16),
            vmem((10, ELEC, 2 * PAD), BF16),
            vmem((4, PAD, 512), BF16),
            vmem((PAD, 512), BF16),
            vmem((ELEC, PAD), BF16),
            vmem((4, ELEC, 2 * PAD), BF16),
            vmem((512, PAD), F32),
            vmem((2, PAD), F32),
            vmem((16, 2, PAD), F32),
            vmem((32, 8, 128), F32),
            vmem((4, 8, 256), F32),
            vmem((2, ROWS), F32),
            pltpu.SemaphoreType.DMA((8,)),
            pltpu.SemaphoreType.DMA((FLOWS,)),
            pltpu.SemaphoreType.DMA((FLOWS,)),
            pltpu.SemaphoreType.DMA((16,)),
            pltpu.SemaphoreType.DMA((16,)),
            pltpu.SemaphoreType.DMA((32,)),
            pltpu.SemaphoreType.DMA((32,)),
            pltpu.SemaphoreType.REGULAR((4,)),
        ],
        compiler_params=pltpu.CompilerParams(
            collective_id=0, has_side_effects=True, vmem_limit_bytes=67_000_000),
    )(green_half, collocation, occupied.T, kernel)
    return pl.pallas_call(
        finish,
        out_shape=(jax.ShapeDtypeStruct((2, PTS), F32), jax.ShapeDtypeStruct((2,), F32), jax.ShapeDtypeStruct((2,), F32)),
        in_specs=[in_vmem, in_vmem],
        out_specs=(in_vmem, in_smem, in_smem),
    )(pot, total)


def solution(mesh):
    placed = (P("wlk", None, None), P("wlk", "pts"), P("pts", None), P("pts", None))
    return jax.shard_map(
        local,
        mesh=mesh,
        in_specs=placed,
        out_specs=(P("wlk", "pts"), P("wlk"), P("wlk")),
        check_vma=False,
    )
```

```python
import jax
import jax.numpy as jnp
from jax import lax
from jax.experimental import pallas as pl
from jax.experimental.pallas import tpu as pltpu
from jax.sharding import PartitionSpec as P

MESH = pl.DeviceIdType.MESH
F32, BF16 = jnp.float32, jnp.bfloat16

ELEC = 400
PTS = 600
PAD = 640
ROWS = 608
DEEP = 300
DEEP_PAD = 304
GROUPS = 8
C_CUT = 160
KCH = 160
CHUNK = ((0, 256), (256, 256), (512, 128))
PARTS = range(len(CHUNK))
STEPS = ((0, 2), (2, 4), (4, 5))
FLOWS = 144


def dot(a, b):
    return jnp.dot(a, b, preferred_element_type=F32)


def body(green, colloc, occ, kmat, pot_out, sum_out,
         cin, oin, gv, g8, kst, kb, cbuf, acc, ttown, ttbuf, tp, op, otown, otbuf,
         trans, dens, dbuf, ebuf, exch, pot, local_sem, send, recv, d_send, d_recv, e_send, e_recv, hear):
    a, g = lax.axis_index("pts"), lax.axis_index("wlk")
    zh, x, c = a // 8, (a // 2) % 4, a % 2
    zl, y = g // 4, g % 4
    z = zh * 2 + zl
    is_same = zh == zl
    is_cross = zh != zl
    same = is_same.astype(jnp.int32)

    def at(zz, xx, cc, yy):
        return {"pts": (zz // 2) * 8 + xx * 2 + cc, "wlk": (zz % 2) * 4 + yy}

    sib = at(z, x, 1 - c, y)
    right, left = at(z, (x + 1) % 4, c, y), at(z, (x + 3) % 4, c, y)
    up, down = at(z, x, c, (y + 1) % 4), at(z, x, c, (y + 3) % 4)
    zmate = at(zh * 2 + 1 - zl, x, c, y)
    xmate = at(3 - z, x, c, y)
    lanes = tuple(pl.ds(pl.multiple_of(2 * start + c * size, 128), size) for start, size in CHUNK)
    cols = tuple(pl.ds(start, size) for start, size in CHUNK)
    numbers = iter(range(FLOWS))

    def flow(src, dst, dev):
        f = next(numbers)
        return pltpu.make_async_remote_copy(
            src_ref=src, dst_ref=dst, send_sem=send.at[f], recv_sem=recv.at[f],
            device_id=dev, device_id_type=MESH)

    def start(*copies):
        for cp in copies:
            cp.start()

    load_c = pltpu.make_async_copy(colloc, cin, local_sem.at[0])
    load_o = pltpu.make_async_copy(occ, oin, local_sem.at[1])
    load_g = [pltpu.make_async_copy(green.at[w], gv.at[pl.ds(w * ELEC, ELEC)], local_sem.at[2 + w]) for w in range(2)]
    pieces = [(s, min(KCH, PTS - s)) for s in range(0, PTS, KCH)]
    load_k = [pltpu.make_async_copy(kmat.at[pl.ds(s, n)], kst.at[i % 2, pl.ds(0, n)], local_sem.at[4 + i])
              for i, (s, n) in enumerate(pieces)]
    start(load_c, load_o)

    plane = z * 8 + x * 2 + c

    def plane_dev(r):
        q = (plane + r) % 32
        return at(q // 8, (q // 2) % 4, q % 2, y)

    barrier = pltpu.get_barrier_semaphore()
    for dev in (up, down, right, left, zmate, xmate, sib):
        pl.semaphore_signal(barrier, inc=1, device_id=dev, device_id_type=MESH)

    rounds = ((right, left), (right, left), (zmate, xmate), (sib,))

    def tell(r):
        for dev in rounds[r]:
            pl.semaphore_signal(hear.at[r], inc=1, device_id=dev, device_id_type=MESH)

    def heard(r):
        pl.semaphore_wait(hear.at[r], len(rounds[r]))
        if r + 1 < len(rounds):
            tell(r + 1)
    cbuf[g, :, pl.ds(PAD - 128, 128)] = jnp.zeros((DEEP_PAD, 128), BF16)
    cbuf[g, pl.ds(DEEP_PAD - 16, 16), :] = jnp.zeros((16, PAD), BF16)
    load_c.wait()
    cbuf[g, pl.ds(0, DEEP), pl.ds(0, PTS)] = cin[...]
    start(*load_g)
    load_o.wait()
    otown[:, pl.ds(PAD - 128, 128)] = jnp.zeros((ELEC, 128), BF16)
    otown[:, pl.ds(0, PTS)] = oin[...]

    @pl.when(is_same)
    def _():
        for h in PARTS:
            otbuf[0, :, lanes[h]] = otown[:, cols[h]]

    pl.semaphore_wait(barrier, 7)
    tell(0)

    def slot(zlo, yy):
        return zlo * 4 + yy

    def c_flow(k, h, dev, first=0, count=DEEP_PAD):
        ref = cbuf.at[k, pl.ds(first, count), cols[h]]
        return flow(ref, ref, dev)

    own_k, mate_k = slot(zl, y), slot(1 - zl, y)
    dn, un, on = (y + 3) % 4, (y + 1) % 4, (y + 2) % 4
    c_z, c_own, c_mate, c_far, c_zfar, c_matefar = [], [], [], [], [], []
    for h in PARTS:
        c_z.append(c_flow(own_k, h, zmate))
        c_own.append((c_flow(own_k, h, up), c_flow(own_k, h, down)))
        c_mate.append((c_flow(mate_k, h, up), c_flow(mate_k, h, down)))
        c_far.append((c_flow(slot(zl, dn), h, up, 0, C_CUT),
                      c_flow(slot(zl, un), h, down, C_CUT, DEEP_PAD - C_CUT)))
        if h == 0:
            c_zfar.append(c_flow(slot(zl, on), h, zmate))
        else:
            c_matefar.append((c_flow(slot(1 - zl, dn), h, up, 0, C_CUT),
                              c_flow(slot(1 - zl, un), h, down, C_CUT, DEEP_PAD - C_CUT)))
    start(*c_own[0], c_z[0], *c_own[1], c_z[1], c_z[2])

    def o_block(i, h):
        return otbuf.at[i, :, lanes[h]]

    o_xx = [flow(otown.at[:, cols[h]], o_block(0, h), xmate) for h in PARTS]
    o_right = [flow(o_block(0, h), o_block(1, h), right) for h in PARTS]
    o_left = [flow(o_block(0, h), o_block(2, h), left) for h in PARTS]
    o_sib = [flow(o_block(0, h), o_block(0, h), sib) for h in PARTS]
    o_far = [flow(o_block(1, 0), o_block(3, 0), right), flow(o_block(2, 1), o_block(3, 1), left),
             flow(o_block(1, 2), o_block(3, 2), right)]
    o_relay = [[flow(o_block(i, h), o_block(i, h), sib) for h in PARTS] for i in (1, 2, 3)]
    o_first = o_right + o_left + o_sib

    @pl.when(is_cross)
    def _():
        start(*o_xx)

    @pl.when(is_same)
    def _():
        for h in PARTS:
            start(o_right[h], o_left[h], o_sib[h])

    for cp in load_g:
        cp.wait()
    start(load_k[0], load_k[1])

    def cut_green(r, carry):
        rows = pl.ds(pl.multiple_of(r * 80, 16), 80)
        piece = gv[rows, :]
        for k in range(GROUPS):
            part = piece[:, k * DEEP:(k + 1) * DEEP]
            g8[k, rows, pl.ds(0, DEEP_PAD)] = jnp.concatenate([part, jnp.zeros((80, DEEP_PAD - DEEP), BF16)], axis=1)
        return carry

    lax.fori_loop(0, 10, cut_green, 0)
    heard(0)

    def add_theta(k, h, first=False):
        part = dot(g8[k, :, pl.ds(0, DEEP_PAD)], cbuf[k, :, cols[h]])
        if first:
            acc[:, cols[h]] = part
        else:
            acc[:, cols[h]] += part

    def cut_kernel(i):
        s, n = pieces[i]
        load_k[i].wait()

        def rows_at(r, carry):
            rows = pl.ds(pl.multiple_of(r * 16, 16), 16)
            out = pl.ds(pl.multiple_of(s + r * 16, 16), 16)
            for b in range(16):
                j, core = b // 2, b % 2
                kb[j, out, pl.ds(core * 256, 256)] = kst[i % 2, rows, pl.ds(b * PTS, 256)]
                kb[j, out, pl.ds(512 + core * 256, 256)] = kst[i % 2, rows, pl.ds(b * PTS + 256, 256)]
                part = kst[i % 2, rows, pl.ds(b * PTS + 512, PTS - 512)]
                kb[j, out, pl.ds(1024 + core * 128, 128)] = jnp.concatenate(
                    [part, jnp.zeros((16, PAD - PTS), BF16)], axis=1)
            return carry

        lax.fori_loop(0, (n + 15) // 16, rows_at, 0)
        if i + 2 < len(pieces):
            load_k[i + 2].start()

    def take(pair):
        for cp in pair:
            cp.wait_recv()

    def near_arrives(h):
        c_own[h][0].wait_recv()
        c_far[h][0].start()
        c_own[h][1].wait_recv()
        c_far[h][1].start()
        c_z[h].wait_recv()
        start(*c_mate[h])

    def far_arrives(h):
        take(c_far[h])
        if h == 0:
            c_zfar[0].start()

    for h in PARTS:
        add_theta(own_k, h, True)
    def occupied_part(h):
        o_right[h].wait_recv()
        o_left[h].wait_recv()
        start(o_far[h], o_relay[0][h], o_relay[1][h])

    def occupied_from_z(h):
        o_xx[h].wait_recv()
        start(o_right[h], o_left[h], o_sib[h])

    def add_near(h):
        add_theta(slot(zl, dn), h)
        add_theta(slot(zl, un), h)
        add_theta(mate_k, h)

    def add_mates(h):
        take(c_mate[h])
        if h:
            start(*c_matefar[h - 1])
        add_theta(slot(1 - zl, dn), h)
        add_theta(slot(1 - zl, un), h)

    cut_kernel(0)
    heard(1)
    near_arrives(0)
    start(*c_own[2])

    @pl.when(is_cross)
    def _():
        occupied_from_z(0)

    add_near(0)
    cut_kernel(1)
    near_arrives(1)

    @pl.when(is_cross)
    def _():
        occupied_from_z(1)

    far_arrives(0)

    @pl.when(is_same)
    def _():
        occupied_part(0)

    add_theta(slot(zl, on), 0)
    heard(2)
    add_near(1)

    @pl.when(is_cross)
    def _():
        occupied_from_z(2)

    @pl.when(is_same)
    def _():
        occupied_part(1)
        occupied_part(2)

    cut_kernel(3)
    add_mates(0)
    c_zfar[0].wait_recv()
    add_theta(slot(1 - zl, on), 0)

    def t_block(i, h):
        return ttbuf.at[i, :, lanes[h]]

    def t_flows(count, make):
        return [[make(w, h) for h in PARTS] for w in range(count)]

    t_z = t_flows(2, lambda w, h: flow(ttown.at[w, :, cols[h]], t_block(2 + w, h), zmate))
    t_xx = t_flows(2, lambda w, h: flow(ttown.at[w, :, cols[h]], t_block(w, h), xmate))
    t_sib = t_flows(2, lambda w, h: flow(t_block(w, h), t_block(w, h), sib))
    t_sibz = t_flows(2, lambda w, h: flow(t_block(2 + w, h), t_block(2 + w, h), sib))
    t_right = t_flows(2, lambda w, h: flow(t_block(w * (1 + same), h), t_block(4 + w, h), right))
    t_left = t_flows(2, lambda w, h: flow(t_block(same + w * (1 + same), h), t_block(6 + w, h), left))
    low_r = (x + 1) % 4 < 2
    low_l = (x + 3) % 4 < 2
    go_r = 4 + jnp.where(is_same & jnp.logical_not(low_r), 1, 0)
    go_l = 6 + jnp.where(is_same & low_l, 0, 1)
    t_far = [[flow(t_block(go_r, h), t_block(8, h), right) for h in PARTS],
             [flow(t_block(go_l, h), t_block(9, h), left) for h in PARTS]]
    t_relay = [[flow(t_block(i, h), t_block(i, h), sib) for h in PARTS] for i in range(4, 10)]

    def turned(src, size):
        trans[pl.ds(0, ELEC), pl.ds(0, size)] = src.astype(F32)
        return jnp.swapaxes(trans[:, pl.ds(0, size)], 0, 1).astype(BF16)

    def turn(side, h):
        tp[side, cols[h], :] = turned(ttbuf[side, :, lanes[h]], CHUNK[h][1])

    def cross_go(w, h):
        t_xx[w][h].wait_recv()
        start(t_right[w][h], t_left[w][h], t_sib[w][h])

    def same_go(w, h):
        t_z[w][h].wait_recv()
        start(t_right[1][h] if w == 0 else t_left[1][h], t_sibz[w][h])
        turn(2 + w, h)

    def d_flow(r):
        return pltpu.make_async_remote_copy(
            src_ref=dbuf.at[a], dst_ref=dbuf.at[a], send_sem=d_send.at[r], recv_sem=d_recv.at[r],
            device_id={"pts": (a + r) % 16, "wlk": g}, device_id_type=MESH)

    def d_start(r, carry):
        d_flow(r).start()
        return carry

    def d_wait(r, carry):
        d_flow(r).wait()
        return carry

    def publish(h):
        for w in range(2):
            t = acc[pl.ds(w * ELEC, ELEC), cols[h]].astype(BF16)
            ttown[w, :, cols[h]] = t

            @pl.when(is_same)
            def _():
                ttbuf[w, :, lanes[h]] = t

            dens[pl.ds(w, 1), cols[h]] = jnp.sum(
                t.astype(F32) * otown[:, cols[h]].astype(F32), axis=0, keepdims=True)

        if h == 2:
            dbuf[a] = dens[...].astype(BF16).astype(F32)
            lax.fori_loop(1, 16, d_start, 0)

        @pl.when(is_same)
        def _():
            start(t_right[0][h], t_left[0][h], t_z[0][h], t_sib[0][h], t_sib[1][h])
            if h == 2:
                start(*t_z[1])

        @pl.when(is_cross)
        def _():
            if h == 1:
                start(t_xx[0][1], t_z[0][1])
            elif h == 0:
                start(t_xx[0][0], t_z[0][0], t_xx[1][0], t_z[1][0])
            else:
                start(t_xx[1][1], t_z[1][1], t_xx[0][2], t_z[0][2], t_xx[1][2], t_z[1][2])

    publish(0)
    heard(3)

    near_arrives(2)
    far_arrives(1)

    @pl.when(is_cross)
    def _():
        occupied_part(0)

    @pl.when(is_cross)
    def _():
        occupied_part(1)

    add_theta(slot(zl, on), 1)
    cut_kernel(2)
    add_mates(1)
    far_arrives(2)

    @pl.when(is_cross)
    def _():
        occupied_part(2)

    add_near(2)
    add_theta(slot(zl, on), 2)

    @pl.when(is_cross)
    def _():
        cross_go(0, 0)

    add_mates(2)
    take(c_matefar[0])
    add_theta(slot(1 - zl, on), 1)
    publish(1)

    take(c_matefar[1])
    add_theta(slot(1 - zl, on), 2)
    publish(2)

    @pl.when(is_same)
    def _():
        same_go(0, 0)

    def potential(first):
        if first == 0:
            pot[...] = jnp.zeros_like(pot)

        def add_chip(j, carry):
            one, two = dbuf[2 * j].astype(BF16), dbuf[2 * j + 1].astype(BF16)
            both = jnp.concatenate([v[:, i:i + n] for i, n in CHUNK for v in (one, two)], axis=1)
            pot[...] += lax.dot_general(both, kb[j], (((1,), (1,)), ((), ())), preferred_element_type=F32)
            return carry

        lax.fori_loop(first, first + 4, add_chip, 0)
        if first:
            pot_out[...] = pot[:, pl.ds(0, PTS)]

    exch[...] = jnp.zeros_like(exch)

    def unit(tt, side, ot, chip, weight, h):
        left_t = tp[side, pl.ds(0, ROWS), pl.ds(0, ELEC)]
        left_o = op[pl.ds(0, ROWS), pl.ds(0, ELEC)]

        def step(n, carry):
            part = pl.ds(n * 256, 256)
            near = dot(left_t, otbuf[ot, :, part])
            away = dot(left_o, ttbuf[tt, :, part])
            terms = kb[chip, :, part].astype(F32) * near * away
            return carry + terms.reshape(ROWS // 8, 8, 256).sum(axis=0)

        total = jnp.zeros((8, 256), F32)
        for n in range(*STEPS[h]):
            total = step(n, total)
        exch[side] += weight * total

    def z_take(w, h):
        t_z[w][h].wait_recv()
        turn(2 + w, h)

    def from_left(w, h):
        t_right[w][h].wait_recv()
        t_relay[w][h].start()

    def from_right(w, h):
        t_left[w][h].wait_recv()
        t_relay[2 + w][h].start()

    def from_both(w, h):
        from_left(w, h)
        from_right(w, h)

    def from_far(w, h):
        t_far[w][h].wait_recv()
        t_relay[4 + w][h].start()

    base = jnp.where(is_same, zh, 1 - zh) * 4
    of_same = {0: (0, 0, 0, 1.0), 1: (1, 0, 0, 1.0), 2: (2, 0, 0, 1.0), 3: (3, 0, 0, 1.0),
               4: (0, 1, 3, 2.0), 5: (2, 1, 3, 2.0), 6: (1, 2, 1, 2.0), 7: (3, 2, 1, 2.0),
               8: (2 * (x // 2), 3, 2, 2.0), 9: (2 * (x // 2) + 1, 3, 2, 2.0)}
    of_cross = {0: (2, 0, 0, 2.0), 1: (3, 0, 0, 2.0), 4: (2, 1, 3, 2.0), 5: (3, 1, 3, 2.0),
                6: (2, 2, 1, 2.0), 7: (3, 2, 1, 2.0), 8: (2, 3, 2, 2.0), 9: (3, 3, 2, 2.0)}

    def handed(i, h):
        return t_sib[i][h] if i < 2 else t_sibz[i - 2][h] if i < 4 else t_relay[i - 4][h]

    def run(s_block, x_block, h):
        @pl.when(is_same)
        def _():
            handed(s_block, h).wait_recv()

        @pl.when(is_cross)
        def _():
            handed(x_block, h).wait_recv()

        picked = [jnp.where(is_same, u, v) for u, v in zip((s_block, *of_same[s_block]), (x_block, *of_cross[x_block]))]
        unit(picked[0], picked[1], picked[2], base + (x + picked[3]) % 4, picked[4], h)

    def own(i, h):
        handed(i, h).wait_recv()
        side, ot, away, weight = of_same[i]
        unit(i, side, ot, base + (x + away) % 4, weight, h)

    op[...] = turned(otown[...], PAD)

    @pl.when(is_cross)
    def _():
        cross_go(1, 0)

    @pl.when(is_same)
    def _():
        same_go(1, 0)
        from_both(0, 0)

    kb[:, pl.ds(PTS, ROWS - PTS), :] = jnp.zeros((8, ROWS - PTS, 2 * PAD), BF16)
    take(o_sib)

    @pl.when(is_same)
    def _():
        for w in range(2):
            for h in PARTS:
                turn(w, h)
        own(0, 0)
        own(0, 1)
        own(0, 2)
        same_go(0, 1)
        from_both(0, 1)
        own(1, 0)
        own(1, 1)
        own(1, 2)

    @pl.when(is_cross)
    def _():
        z_take(0, 0)
        from_both(0, 0)
        cross_go(0, 1)
        z_take(0, 1)

    take(o_far)
    start(*o_relay[2])
    lax.fori_loop(1, 16, d_wait, 0)
    potential(0)

    @pl.when(is_same)
    def _():
        same_go(1, 1)
        from_left(1, 0)
        t_far[0][0].start()

    @pl.when(is_cross)
    def _():
        from_both(1, 0)
        cross_go(1, 1)
        start(t_far[0][0], t_far[1][0])
        z_take(0, 2)

    potential(4)
    for part in o_relay:
        take(part)
    run(4, 0, 0)
    run(4, 0, 1)

    @pl.when(is_same)
    def _():
        same_go(0, 2)
        from_both(0, 2)
        from_right(1, 0)
        t_far[1][0].start()

    @pl.when(is_cross)
    def _():
        cross_go(0, 2)

    run(6, 4, 0)

    @pl.when(is_cross)
    def _():
        cross_go(1, 2)

    run(2, 6, 0)

    @pl.when(is_same)
    def _():
        same_go(1, 2)

    @pl.when(is_cross)
    def _():
        from_both(0, 1)
        t_far[0][1].start()

    run(4, 0, 2)

    @pl.when(is_same)
    def _():
        from_left(1, 1)
        t_far[0][1].start()

    run(6, 4, 1)

    @pl.when(is_cross)
    def _():
        z_take(1, 0)
        z_take(1, 1)

    run(2, 6, 1)

    @pl.when(is_same)
    def _():
        from_right(1, 1)
        t_far[1][1].start()

    @pl.when(is_cross)
    def _():
        z_take(1, 2)

    run(3, 1, 0)
    run(3, 1, 1)

    @pl.when(is_cross)
    def _():
        from_both(1, 1)
        t_far[1][1].start()

    run(5, 5, 0)
    run(7, 7, 0)

    @pl.when(is_same)
    def _():
        from_left(1, 2)
        t_far[0][2].start()

    run(6, 1, 2)
    from_far(0, 0)

    @pl.when(is_cross)
    def _():
        from_both(0, 2)
        t_far[0][2].start()

    @pl.when(is_same)
    def _():
        from_right(1, 2)
        t_far[1][2].start()

    run(5, 5, 1)
    run(8, 8, 0)
    from_far(1, 0)

    @pl.when(is_cross)
    def _():
        from_both(1, 2)
        t_far[1][2].start()

    run(7, 7, 1)
    run(9, 9, 0)
    run(2, 4, 2)
    run(3, 6, 2)
    run(5, 5, 2)
    from_far(0, 1)
    run(7, 7, 2)
    from_far(1, 1)
    run(8, 8, 1)
    from_far(0, 2)
    run(9, 9, 1)
    from_far(1, 2)
    run(8, 8, 2)
    run(9, 9, 2)

    row = lax.broadcasted_iota(jnp.int32, (8, 128), 0)
    tile = jnp.zeros((8, 128), F32)
    for side in range(4):
        tile = jnp.where(row == (zl * 2 + side) % 4, -0.5 * jnp.sum(exch[side]), tile)
    for w in range(2):
        tile = jnp.where(row == 4 + zl * 2 + w,
                         0.5 * jnp.sum(dens[pl.ds(w, 1), pl.ds(0, PTS)] * pot[pl.ds(w, 1), pl.ds(0, PTS)]), tile)
    ebuf[plane] = tile

    def e_flow(r):
        return pltpu.make_async_remote_copy(
            src_ref=ebuf.at[plane], dst_ref=ebuf.at[plane], send_sem=e_send.at[r], recv_sem=e_recv.at[r],
            device_id=plane_dev(r), device_id_type=MESH)

    def e_wait(r, carry):
        e_flow(r).wait()
        return carry

    for r in (*range(16, 32), *range(15, 0, -1)):
        e_flow(r).start()

    for pairs in (c_own, c_mate, c_far, c_matefar, t_z, t_right, t_left, t_sib, t_far, t_relay, o_relay):
        for pair in pairs:
            for cp in pair:
                cp.wait_send()
    for cp in c_z + c_zfar + o_first + o_far:
        cp.wait_send()

    @pl.when(is_cross)
    def _():
        for cp in o_xx + t_xx[0] + t_xx[1]:
            cp.wait_send()

    @pl.when(is_same)
    def _():
        for cp in t_sibz[0] + t_sibz[1]:
            cp.wait_send()

    lax.fori_loop(1, 32, e_wait, 0)
    sum_out[...] = ebuf[...].sum(axis=0)


def finish(pot, total, pot_out, cou_out, exc_out):
    zl = lax.axis_index("wlk") // 4
    pot_out[...] = pot[...]
    row = lax.broadcasted_iota(jnp.int32, (8, 128), 0)
    for w in range(2):
        exc_out[w] = jnp.sum(jnp.where(row == zl * 2 + w, total[...], 0.0)) * (1.0 / 128)
        cou_out[w] = jnp.sum(jnp.where(row == 4 + zl * 2 + w, total[...], 0.0)) * (1.0 / 128)


def local(green_half, collocation, occupied, kernel):
    any_space = pl.BlockSpec(memory_space=pl.ANY)
    vmem = pltpu.VMEM
    in_vmem, in_smem = pl.BlockSpec(memory_space=vmem), pl.BlockSpec(memory_space=pltpu.SMEM)
    pot, total = pl.pallas_call(
        body,
        out_shape=(jax.ShapeDtypeStruct((2, PTS), F32), jax.ShapeDtypeStruct((8, 128), F32)),
        in_specs=[any_space] * 4,
        out_specs=(in_vmem, in_vmem),
        scratch_shapes=[
            vmem((DEEP, PTS), BF16),
            vmem((ELEC, PTS), BF16),
            vmem((2 * ELEC, 8 * DEEP), BF16),
            vmem((GROUPS, 2 * ELEC, 384), BF16),
            vmem((2, KCH, 16 * PTS), BF16),
            vmem((8, ROWS, 2 * PAD), BF16),
            vmem((GROUPS, DEEP_PAD, PAD), BF16),
            vmem((2 * ELEC, PAD), F32),
            vmem((2, ELEC, PAD), BF16),
            vmem((10, ELEC, 2 * PAD), BF16),
            vmem((4, PAD, 512), BF16),
            vmem((PAD, 512), BF16),
            vmem((ELEC, PAD), BF16),
            vmem((4, ELEC, 2 * PAD), BF16),
            vmem((512, PAD), F32),
            vmem((2, PAD), F32),
            vmem((16, 2, PAD), F32),
            vmem((32, 8, 128), F32),
            vmem((4, 8, 256), F32),
            vmem((2, ROWS), F32),
            pltpu.SemaphoreType.DMA((8,)),
            pltpu.SemaphoreType.DMA((FLOWS,)),
            pltpu.SemaphoreType.DMA((FLOWS,)),
            pltpu.SemaphoreType.DMA((16,)),
            pltpu.SemaphoreType.DMA((16,)),
            pltpu.SemaphoreType.DMA((32,)),
            pltpu.SemaphoreType.DMA((32,)),
            pltpu.SemaphoreType.REGULAR((4,)),
        ],
        compiler_params=pltpu.CompilerParams(
            collective_id=0, has_side_effects=True, vmem_limit_bytes=67_000_000),
    )(green_half, collocation, occupied.T, kernel)
    return pl.pallas_call(
        finish,
        out_shape=(jax.ShapeDtypeStruct((2, PTS), F32), jax.ShapeDtypeStruct((2,), F32), jax.ShapeDtypeStruct((2,), F32)),
        in_specs=[in_vmem, in_vmem],
        out_specs=(in_vmem, in_smem, in_smem),
    )(pot, total)


def solution(mesh):
    placed = (P("wlk", None, None), P("wlk", "pts"), P("pts", None), P("pts", None))
    return jax.shard_map(
        local,
        mesh=mesh,
        in_specs=placed,
        out_specs=(P("wlk", "pts"), P("wlk"), P("wlk")),
        check_vma=False,
    )
```

```python
import jax
import jax.numpy as jnp
from jax import lax
from jax.experimental import pallas as pl
from jax.experimental.pallas import tpu as pltpu
from jax.sharding import PartitionSpec as P

MESH = pl.DeviceIdType.MESH
F32, BF16 = jnp.float32, jnp.bfloat16

ELEC = 400
PTS = 600
PAD = 640
ROWS = 608
DEEP = 300
DEEP_PAD = 304
GROUPS = 8
C_CUT = 160
KCH = 160
CHUNK = ((0, 256), (256, 256), (512, 128))
PARTS = range(len(CHUNK))
STEPS = ((0, 2), (2, 4), (4, 5))
FLOWS = 110


def dot(a, b):
    return jnp.dot(a, b, preferred_element_type=F32)


def body(green, colloc, occ, kmat, pot_out, sum_out,
         cin, oin, gv, g8, kst, kb, cbuf, acc, ttown, ttbuf, tp, op, otown, otbuf,
         trans, dens, dbuf, ebuf, exch, pot, local_sem, send, recv, d_sem, e_sem, hear, pot_all):
    a, g = lax.axis_index("pts"), lax.axis_index("wlk")
    zh, x, c = a // 8, (a // 2) % 4, a % 2
    zl, y = g // 4, g % 4
    z = zh * 2 + zl
    is_same = zh == zl
    is_cross = zh != zl
    same = is_same.astype(jnp.int32)

    def at(zz, xx, cc, yy):
        return {"pts": (zz // 2) * 8 + xx * 2 + cc, "wlk": (zz % 2) * 4 + yy}

    sib = at(z, x, 1 - c, y)
    right, left = at(z, (x + 1) % 4, c, y), at(z, (x + 3) % 4, c, y)
    up, down = at(z, x, c, (y + 1) % 4), at(z, x, c, (y + 3) % 4)
    zmate = at(zh * 2 + 1 - zl, x, c, y)
    xmate = at(3 - z, x, c, y)
    lanes = tuple(pl.ds(pl.multiple_of(2 * start + c * size, 128), size) for start, size in CHUNK)
    cols = tuple(pl.ds(start, size) for start, size in CHUNK)
    numbers = iter(range(FLOWS))

    def flow(src, dst, dev, group):
        return pltpu.make_async_remote_copy(
            src_ref=src, dst_ref=dst, send_sem=send.at[group], recv_sem=recv.at[next(numbers)],
            device_id=dev, device_id_type=MESH)

    def sent(group, ref):
        pltpu.make_async_remote_copy(
            src_ref=ref, dst_ref=ref, send_sem=send.at[group], recv_sem=recv.at[0],
            device_id=sib, device_id_type=MESH).wait_send()

    def start(*copies):
        for cp in copies:
            cp.start()

    load_c = pltpu.make_async_copy(colloc, cin, local_sem.at[0])
    load_o = pltpu.make_async_copy(occ, oin, local_sem.at[1])
    load_g = [pltpu.make_async_copy(green.at[w], gv.at[pl.ds(w * ELEC, ELEC)], local_sem.at[2 + w]) for w in range(2)]
    pieces = [(s, min(KCH, PTS - s)) for s in range(0, PTS, KCH)]
    load_k = [pltpu.make_async_copy(kmat.at[pl.ds(s, n)], kst.at[i % 2, pl.ds(0, n)], local_sem.at[4 + i])
              for i, (s, n) in enumerate(pieces)]
    start(load_c, load_o)

    plane = z * 8 + x * 2 + c

    def plane_dev(r):
        q = (plane + r) % 32
        return at(q // 8, (q // 2) % 4, q % 2, y)

    barrier = pltpu.get_barrier_semaphore()
    for dev in (up, down, right, left, zmate, xmate, sib):
        pl.semaphore_signal(barrier, inc=1, device_id=dev, device_id_type=MESH)

    rounds = ((right, left), (right, left), (zmate, xmate), (sib,))

    def tell(r):
        for dev in rounds[r]:
            pl.semaphore_signal(hear.at[r], inc=1, device_id=dev, device_id_type=MESH)

    def heard(r):
        pl.semaphore_wait(hear.at[r], len(rounds[r]))
        if r + 1 < len(rounds):
            tell(r + 1)
    cbuf[g, :, pl.ds(PAD - 128, 128)] = jnp.zeros((DEEP_PAD, 128), BF16)
    cbuf[g, pl.ds(DEEP_PAD - 16, 16), :] = jnp.zeros((16, PAD), BF16)
    load_c.wait()
    cbuf[g, pl.ds(0, DEEP), pl.ds(0, PTS)] = cin[...]
    start(*load_g)
    load_o.wait()
    otown[:, pl.ds(PAD - 128, 128)] = jnp.zeros((ELEC, 128), BF16)
    otown[:, pl.ds(0, PTS)] = oin[...]

    @pl.when(is_same)
    def _():
        for h in PARTS:
            otbuf[0, :, lanes[h]] = otown[:, cols[h]]

    pl.semaphore_wait(barrier, 7)
    tell(0)

    def slot(zlo, yy):
        return zlo * 4 + yy

    def c_flow(group, k, h, dev, first=0, count=DEEP_PAD):
        ref = cbuf.at[k, pl.ds(first, count), cols[h]]
        return flow(ref, ref, dev, group)

    own_k, mate_k = slot(zl, y), slot(1 - zl, y)
    dn, un, on = (y + 3) % 4, (y + 1) % 4, (y + 2) % 4
    c_z, c_own, c_mate, c_far, c_zfar, c_matefar = [], [], [], [], [], []
    for h in PARTS:
        c_z.append(c_flow(0, own_k, h, zmate))
        c_own.append((c_flow(1, own_k, h, up), c_flow(1, own_k, h, down)))
        c_mate.append((c_flow(2, mate_k, h, up), c_flow(2, mate_k, h, down)))
        c_far.append((c_flow(3, slot(zl, dn), h, up, 0, C_CUT),
                      c_flow(3, slot(zl, un), h, down, C_CUT, DEEP_PAD - C_CUT)))
        if h == 0:
            c_zfar.append(c_flow(4, slot(zl, on), h, zmate))
        else:
            c_matefar.append((c_flow(5, slot(1 - zl, dn), h, up, 0, C_CUT),
                              c_flow(5, slot(1 - zl, un), h, down, C_CUT, DEEP_PAD - C_CUT)))
    start(*c_own[0], c_z[0], *c_own[1], c_z[1], c_z[2])

    def o_block(i, h):
        return otbuf.at[i, :, lanes[h]]

    o_xx = [flow(otown.at[:, cols[h]], o_block(0, h), xmate, 6) for h in PARTS]
    o_right = [flow(o_block(0, h), o_block(1, h), right, 7) for h in PARTS]
    o_left = [flow(o_block(0, h), o_block(2, h), left, 8) for h in PARTS]
    o_sib = [flow(o_block(0, h), o_block(0, h), sib, 9) for h in PARTS]
    o_far = [flow(o_block(1, 0), o_block(3, 0), right, 10), flow(o_block(2, 1), o_block(3, 1), left, 10),
             flow(o_block(1, 2), o_block(3, 2), right, 10)]
    o_relay = [[flow(o_block(i, h), o_block(i, h), sib, 11 + i // 3) for h in PARTS] for i in (1, 2, 3)]
    o_first = o_right + o_left + o_sib

    @pl.when(is_cross)
    def _():
        start(*o_xx)

    @pl.when(is_same)
    def _():
        for h in PARTS:
            start(o_right[h], o_left[h], o_sib[h])

    for cp in load_g:
        cp.wait()
    start(load_k[0], load_k[1])

    def cut_green(r, carry):
        rows = pl.ds(pl.multiple_of(r * 80, 16), 80)
        piece = gv[rows, :]
        for k in range(GROUPS):
            part = piece[:, k * DEEP:(k + 1) * DEEP]
            g8[k, rows, pl.ds(0, DEEP_PAD)] = jnp.concatenate([part, jnp.zeros((80, DEEP_PAD - DEEP), BF16)], axis=1)
        return carry

    lax.fori_loop(0, 10, cut_green, 0)
    heard(0)

    def add_theta(k, h, first=False):
        part = dot(g8[k, :, pl.ds(0, DEEP_PAD)], cbuf[k, :, cols[h]])
        if first:
            acc[:, cols[h]] = part
        else:
            acc[:, cols[h]] += part

    def cut_kernel(i):
        s, n = pieces[i]
        load_k[i].wait()

        def rows_at(r, carry):
            rows = pl.ds(pl.multiple_of(r * 16, 16), 16)
            out = pl.ds(pl.multiple_of(s + r * 16, 16), 16)
            for b in range(16):
                j, core = b // 2, b % 2
                kb[j, out, pl.ds(core * 256, 256)] = kst[i % 2, rows, pl.ds(b * PTS, 256)]
                kb[j, out, pl.ds(512 + core * 256, 256)] = kst[i % 2, rows, pl.ds(b * PTS + 256, 256)]
                part = kst[i % 2, rows, pl.ds(b * PTS + 512, PTS - 512)]
                kb[j, out, pl.ds(1024 + core * 128, 128)] = jnp.concatenate(
                    [part, jnp.zeros((16, PAD - PTS), BF16)], axis=1)
            return carry

        lax.fori_loop(0, (n + 15) // 16, rows_at, 0)
        if i + 2 < len(pieces):
            load_k[i + 2].start()

    def take(pair):
        for cp in pair:
            cp.wait_recv()

    def near_arrives(h):
        c_own[h][0].wait_recv()
        c_far[h][0].start()
        c_own[h][1].wait_recv()
        c_far[h][1].start()
        c_z[h].wait_recv()
        start(*c_mate[h])

    def far_arrives(h):
        take(c_far[h])
        if h == 0:
            c_zfar[0].start()

    for h in PARTS:
        add_theta(own_k, h, True)
    def occupied_part(h):
        o_right[h].wait_recv()
        o_left[h].wait_recv()
        start(o_far[h], o_relay[0][h], o_relay[1][h])

    def occupied_from_z(h):
        o_xx[h].wait_recv()
        start(o_right[h], o_left[h], o_sib[h])

    def add_near(h):
        add_theta(slot(zl, dn), h)
        add_theta(slot(zl, un), h)
        add_theta(mate_k, h)

    def add_mates(h):
        take(c_mate[h])
        if h:
            start(*c_matefar[h - 1])
        add_theta(slot(1 - zl, dn), h)
        add_theta(slot(1 - zl, un), h)

    cut_kernel(0)
    heard(1)
    near_arrives(0)
    start(*c_own[2])

    @pl.when(is_cross)
    def _():
        occupied_from_z(0)

    add_near(0)
    cut_kernel(1)
    near_arrives(1)

    @pl.when(is_cross)
    def _():
        occupied_from_z(1)

    far_arrives(0)

    @pl.when(is_same)
    def _():
        occupied_part(0)

    add_theta(slot(zl, on), 0)
    heard(2)
    add_near(1)

    @pl.when(is_cross)
    def _():
        occupied_from_z(2)

    @pl.when(is_same)
    def _():
        occupied_part(1)
        occupied_part(2)

    cut_kernel(3)
    add_mates(0)
    c_zfar[0].wait_recv()
    add_theta(slot(1 - zl, on), 0)

    def t_block(i, h):
        return ttbuf.at[i, :, lanes[h]]

    def t_flows(count, make):
        return [[make(w, h) for h in PARTS] for w in range(count)]

    t_z = t_flows(2, lambda w, h: flow(ttown.at[w, :, cols[h]], t_block(2 + w, h), zmate, 13))
    t_xx = t_flows(2, lambda w, h: flow(ttown.at[w, :, cols[h]], t_block(w, h), xmate, 14))
    t_sib = t_flows(2, lambda w, h: flow(t_block(w, h), t_block(w, h), sib, 15))
    t_sibz = t_flows(2, lambda w, h: flow(t_block(2 + w, h), t_block(2 + w, h), sib, 16))
    t_right = t_flows(2, lambda w, h: flow(t_block(w * (1 + same), h), t_block(4 + w, h), right, 17))
    t_left = t_flows(2, lambda w, h: flow(t_block(same + w * (1 + same), h), t_block(6 + w, h), left, 18))
    low_r = (x + 1) % 4 < 2
    low_l = (x + 3) % 4 < 2
    go_r = 4 + jnp.where(is_same & jnp.logical_not(low_r), 1, 0)
    go_l = 6 + jnp.where(is_same & low_l, 0, 1)
    t_far = [[flow(t_block(go_r, h), t_block(8, h), right, 19) for h in PARTS],
             [flow(t_block(go_l, h), t_block(9, h), left, 19) for h in PARTS]]
    t_relay = [[flow(t_block(i, h), t_block(i, h), sib, 20) for h in PARTS] for i in range(4, 10)]

    def turned(src, size):
        trans[pl.ds(0, ELEC), pl.ds(0, size)] = src.astype(F32)
        return jnp.swapaxes(trans[:, pl.ds(0, size)], 0, 1).astype(BF16)

    def turn(side, h):
        tp[side, cols[h], :] = turned(ttbuf[side, :, lanes[h]], CHUNK[h][1])

    def cross_go(w, h):
        t_xx[w][h].wait_recv()
        start(t_right[w][h], t_left[w][h], t_sib[w][h])

    def same_go(w, h):
        t_z[w][h].wait_recv()
        start(t_right[1][h] if w == 0 else t_left[1][h], t_sibz[w][h])
        turn(2 + w, h)

    def d_flow(r):
        return pltpu.make_async_remote_copy(
            src_ref=dbuf.at[a], dst_ref=dbuf.at[a], send_sem=d_sem.at[0], recv_sem=d_sem.at[1],
            device_id={"pts": (a + r) % 16, "wlk": g}, device_id_type=MESH)

    def d_start(r, carry):
        d_flow(r).start()
        return carry

    def d_wait():
        every = dbuf.at[pl.ds(0, 15)]
        pltpu.make_async_remote_copy(
            src_ref=every, dst_ref=every, send_sem=d_sem.at[0], recv_sem=d_sem.at[1],
            device_id=sib, device_id_type=MESH).wait()

    def publish(h):
        for w in range(2):
            t = acc[pl.ds(w * ELEC, ELEC), cols[h]].astype(BF16)
            ttown[w, :, cols[h]] = t

            @pl.when(is_same)
            def _():
                ttbuf[w, :, lanes[h]] = t

            dens[pl.ds(w, 1), cols[h]] = jnp.sum(
                t.astype(F32) * otown[:, cols[h]].astype(F32), axis=0, keepdims=True)

        if h == 2:
            dbuf[a] = dens[...].astype(BF16).astype(F32)
            lax.fori_loop(1, 16, d_start, 0)

        @pl.when(is_same)
        def _():
            start(t_right[0][h], t_left[0][h], t_z[0][h], t_sib[0][h], t_sib[1][h])
            if h == 2:
                start(*t_z[1])

        @pl.when(is_cross)
        def _():
            if h == 1:
                start(t_xx[0][1], t_z[0][1])
            elif h == 0:
                start(t_xx[0][0], t_z[0][0], t_xx[1][0], t_z[1][0])
            else:
                start(t_xx[1][1], t_z[1][1], t_xx[0][2], t_z[0][2], t_xx[1][2], t_z[1][2])

    publish(0)
    heard(3)

    near_arrives(2)
    far_arrives(1)

    @pl.when(is_cross)
    def _():
        occupied_part(0)

    @pl.when(is_cross)
    def _():
        occupied_part(1)

    add_theta(slot(zl, on), 1)
    cut_kernel(2)
    add_mates(1)
    far_arrives(2)

    @pl.when(is_cross)
    def _():
        occupied_part(2)

    add_near(2)
    add_theta(slot(zl, on), 2)

    @pl.when(is_cross)
    def _():
        cross_go(0, 0)

    add_mates(2)
    take(c_matefar[0])
    add_theta(slot(1 - zl, on), 1)
    publish(1)

    take(c_matefar[1])
    add_theta(slot(1 - zl, on), 2)
    publish(2)

    @pl.when(is_same)
    def _():
        same_go(0, 0)

    def potential(first):
        if first == 0:
            pot[...] = jnp.zeros_like(pot)

        def add_chip(j, carry):
            one, two = dbuf[2 * j].astype(BF16), dbuf[2 * j + 1].astype(BF16)
            both = jnp.concatenate([v[:, i:i + n] for i, n in CHUNK for v in (one, two)], axis=1)
            pot[...] += lax.dot_general(both, kb[j], (((1,), (1,)), ((), ())), preferred_element_type=F32)
            return carry

        lax.fori_loop(first, first + 4, add_chip, 0)
        if first:
            pot_all[...] = pot[:, pl.ds(0, PTS)]
            save_pot.start()

    save_pot = pltpu.make_async_copy(pot_all, pot_out, local_sem.at[0])
    exch[...] = jnp.zeros_like(exch)

    def unit(tt, side, ot, chip, weight, h):
        left_t = tp[side, pl.ds(0, ROWS), pl.ds(0, ELEC)]
        left_o = op[pl.ds(0, ROWS), pl.ds(0, ELEC)]

        def step(n, carry):
            part = pl.ds(n * 256, 256)
            near = dot(left_t, otbuf[ot, :, part])
            away = dot(left_o, ttbuf[tt, :, part])
            terms = kb[chip, :, part].astype(F32) * near * away
            return carry + terms.reshape(ROWS // 8, 8, 256).sum(axis=0)

        total = jnp.zeros((8, 256), F32)
        for n in range(*STEPS[h]):
            total = step(n, total)
        exch[side] += weight * total

    def z_take(w, h):
        t_z[w][h].wait_recv()
        turn(2 + w, h)

    def from_left(w, h):
        t_right[w][h].wait_recv()
        t_relay[w][h].start()

    def from_right(w, h):
        t_left[w][h].wait_recv()
        t_relay[2 + w][h].start()

    def from_both(w, h):
        from_left(w, h)
        from_right(w, h)

    def from_far(w, h):
        t_far[w][h].wait_recv()
        t_relay[4 + w][h].start()

    base = jnp.where(is_same, zh, 1 - zh) * 4
    of_same = {0: (0, 0, 0, 1.0), 1: (1, 0, 0, 1.0), 2: (2, 0, 0, 1.0), 3: (3, 0, 0, 1.0),
               4: (0, 1, 3, 2.0), 5: (2, 1, 3, 2.0), 6: (1, 2, 1, 2.0), 7: (3, 2, 1, 2.0),
               8: (2 * (x // 2), 3, 2, 2.0), 9: (2 * (x // 2) + 1, 3, 2, 2.0)}
    of_cross = {0: (2, 0, 0, 2.0), 1: (3, 0, 0, 2.0), 4: (2, 1, 3, 2.0), 5: (3, 1, 3, 2.0),
                6: (2, 2, 1, 2.0), 7: (3, 2, 1, 2.0), 8: (2, 3, 2, 2.0), 9: (3, 3, 2, 2.0)}

    def handed(i, h):
        return t_sib[i][h] if i < 2 else t_sibz[i - 2][h] if i < 4 else t_relay[i - 4][h]

    def run(s_block, x_block, h):
        @pl.when(is_same)
        def _():
            handed(s_block, h).wait_recv()

        @pl.when(is_cross)
        def _():
            handed(x_block, h).wait_recv()

        picked = [jnp.where(is_same, u, v) for u, v in zip((s_block, *of_same[s_block]), (x_block, *of_cross[x_block]))]
        unit(picked[0], picked[1], picked[2], base + (x + picked[3]) % 4, picked[4], h)

    def own(i, h):
        handed(i, h).wait_recv()
        side, ot, away, weight = of_same[i]
        unit(i, side, ot, base + (x + away) % 4, weight, h)

    op[...] = turned(otown[...], PAD)

    @pl.when(is_cross)
    def _():
        cross_go(1, 0)

    @pl.when(is_same)
    def _():
        same_go(1, 0)
        from_both(0, 0)

    kb[:, pl.ds(PTS, ROWS - PTS), :] = jnp.zeros((8, ROWS - PTS, 2 * PAD), BF16)
    take(o_sib)

    @pl.when(is_same)
    def _():
        for w in range(2):
            for h in PARTS:
                turn(w, h)
        own(0, 0)
        own(0, 1)
        own(0, 2)
        own(1, 0)
        same_go(0, 1)
        own(1, 1)
        own(1, 2)
        from_both(0, 1)

    @pl.when(is_cross)
    def _():
        z_take(0, 0)
        from_both(0, 0)
        cross_go(0, 1)
        z_take(0, 1)

    take(o_far)
    start(*o_relay[2])
    d_wait()
    potential(0)

    @pl.when(is_same)
    def _():
        same_go(1, 1)

    @pl.when(is_cross)
    def _():
        from_both(1, 0)
        cross_go(1, 1)
        start(t_far[0][0], t_far[1][0])
        z_take(0, 2)

    potential(4)
    for part in o_relay:
        take(part)
    run(4, 0, 0)
    run(4, 0, 1)

    @pl.when(is_same)
    def _():
        from_left(1, 0)
        t_far[0][0].start()
        same_go(0, 2)
        from_both(0, 2)
        from_right(1, 0)
        t_far[1][0].start()

    @pl.when(is_cross)
    def _():
        cross_go(0, 2)

    run(6, 4, 0)

    @pl.when(is_cross)
    def _():
        cross_go(1, 2)

    run(2, 6, 0)

    @pl.when(is_same)
    def _():
        same_go(1, 2)

    @pl.when(is_cross)
    def _():
        from_both(0, 1)
        t_far[0][1].start()

    run(4, 0, 2)

    @pl.when(is_same)
    def _():
        from_left(1, 1)
        t_far[0][1].start()

    run(6, 4, 1)

    @pl.when(is_cross)
    def _():
        z_take(1, 0)
        z_take(1, 1)

    run(2, 6, 1)

    @pl.when(is_same)
    def _():
        from_right(1, 1)
        t_far[1][1].start()

    @pl.when(is_cross)
    def _():
        z_take(1, 2)

    run(3, 1, 0)
    run(3, 1, 1)

    @pl.when(is_cross)
    def _():
        from_both(1, 1)
        t_far[1][1].start()

    run(5, 5, 0)
    run(7, 7, 0)

    @pl.when(is_same)
    def _():
        from_left(1, 2)
        t_far[0][2].start()

    run(6, 1, 2)
    from_far(0, 0)

    @pl.when(is_cross)
    def _():
        from_both(0, 2)
        t_far[0][2].start()

    @pl.when(is_same)
    def _():
        from_right(1, 2)
        t_far[1][2].start()

    run(5, 5, 1)
    run(8, 8, 0)
    from_far(1, 0)

    @pl.when(is_cross)
    def _():
        from_both(1, 2)
        t_far[1][2].start()

    run(7, 7, 1)
    run(9, 9, 0)
    run(2, 4, 2)
    run(3, 6, 2)
    run(5, 5, 2)
    from_far(0, 1)
    run(7, 7, 2)
    from_far(1, 1)
    run(8, 8, 1)
    from_far(0, 2)
    run(9, 9, 1)
    from_far(1, 2)
    run(8, 8, 2)
    run(9, 9, 2)

    row = lax.broadcasted_iota(jnp.int32, (8, 128), 0)
    tile = jnp.zeros((8, 128), F32)
    for side in range(4):
        tile = jnp.where(row == (zl * 2 + side) % 4, -0.5 * jnp.sum(exch[side]), tile)
    for w in range(2):
        tile = jnp.where(row == 4 + zl * 2 + w,
                         0.5 * jnp.sum(dens[pl.ds(w, 1), pl.ds(0, PTS)] * pot[pl.ds(w, 1), pl.ds(0, PTS)]), tile)
    ebuf[plane] = tile

    def e_flow(r):
        return pltpu.make_async_remote_copy(
            src_ref=ebuf.at[plane], dst_ref=ebuf.at[plane], send_sem=e_sem.at[0], recv_sem=e_sem.at[1],
            device_id=plane_dev(r), device_id_type=MESH)

    for r in (*range(16, 32), *range(15, 0, -1)):
        e_flow(r).start()

    for group, ref in ((0, cbuf.at[0]), (1, cbuf.at[pl.ds(0, 2)]), (2, cbuf.at[pl.ds(0, 2)]), (3, cbuf.at[0]),
                       (4, cbuf.at[0, :, cols[0]]), (5, cbuf.at[0, :, pl.ds(256, 384)]),
                       (7, otown), (8, otown), (9, otown), (10, otown), (11, otbuf.at[0]), (12, otown),
                       (13, ttown), (15, ttown), (17, ttown), (18, ttown), (19, ttown), (20, ttbuf.at[pl.ds(0, 3)])):
        sent(group, ref)

    @pl.when(is_cross)
    def _():
        sent(6, otown)
        sent(14, ttown)

    @pl.when(is_same)
    def _():
        sent(16, ttown)

    save_pot.wait()
    every = ebuf.at[pl.ds(0, 31)]
    last = pltpu.make_async_remote_copy(
        src_ref=every, dst_ref=every, send_sem=e_sem.at[0], recv_sem=e_sem.at[1],
        device_id=sib, device_id_type=MESH)
    last.wait()
    sum_out[...] = ebuf[...].sum(axis=0)


def finish(pot, total, pot_out, cou_out, exc_out):
    zl = lax.axis_index("wlk") // 4
    pot_out[...] = pot[...]
    row = lax.broadcasted_iota(jnp.int32, (8, 128), 0)
    for w in range(2):
        exc_out[w] = jnp.sum(jnp.where(row == zl * 2 + w, total[...], 0.0)) * (1.0 / 128)
        cou_out[w] = jnp.sum(jnp.where(row == 4 + zl * 2 + w, total[...], 0.0)) * (1.0 / 128)


def local(green_half, collocation, occupied, kernel):
    any_space = pl.BlockSpec(memory_space=pl.ANY)
    vmem = pltpu.VMEM
    in_vmem, in_smem = pl.BlockSpec(memory_space=vmem), pl.BlockSpec(memory_space=pltpu.SMEM)
    pot, total = pl.pallas_call(
        body,
        out_shape=(jax.ShapeDtypeStruct((2, PTS), F32), jax.ShapeDtypeStruct((8, 128), F32)),
        in_specs=[any_space] * 4,
        out_specs=(any_space, in_vmem),
        scratch_shapes=[
            vmem((DEEP, PTS), BF16),
            vmem((ELEC, PTS), BF16),
            vmem((2 * ELEC, 8 * DEEP), BF16),
            vmem((GROUPS, 2 * ELEC, 384), BF16),
            vmem((2, KCH, 16 * PTS), BF16),
            vmem((8, ROWS, 2 * PAD), BF16),
            vmem((GROUPS, DEEP_PAD, PAD), BF16),
            vmem((2 * ELEC, PAD), F32),
            vmem((2, ELEC, PAD), BF16),
            vmem((10, ELEC, 2 * PAD), BF16),
            vmem((4, PAD, 512), BF16),
            vmem((PAD, 512), BF16),
            vmem((ELEC, PAD), BF16),
            vmem((4, ELEC, 2 * PAD), BF16),
            vmem((512, PAD), F32),
            vmem((2, PAD), F32),
            vmem((16, 2, PAD), F32),
            vmem((32, 8, 128), F32),
            vmem((4, 8, 256), F32),
            vmem((2, ROWS), F32),
            pltpu.SemaphoreType.DMA((8,)),
            pltpu.SemaphoreType.DMA((21,)),
            pltpu.SemaphoreType.DMA((FLOWS,)),
            pltpu.SemaphoreType.DMA((2,)),
            pltpu.SemaphoreType.DMA((2,)),
            pltpu.SemaphoreType.REGULAR((4,)),
            vmem((2, PTS), F32),
        ],
        compiler_params=pltpu.CompilerParams(
            collective_id=0, has_side_effects=True, vmem_limit_bytes=67_000_000),
    )(green_half, collocation, occupied.T, kernel)
    return pl.pallas_call(
        finish,
        out_shape=(jax.ShapeDtypeStruct((2, PTS), F32), jax.ShapeDtypeStruct((2,), F32), jax.ShapeDtypeStruct((2,), F32)),
        in_specs=[in_vmem, in_vmem],
        out_specs=(in_vmem, in_smem, in_smem),
    )(pot, total)


def solution(mesh):
    placed = (P("wlk", None, None), P("wlk", "pts"), P("pts", None), P("pts", None))
    return jax.shard_map(
        local,
        mesh=mesh,
        in_specs=placed,
        out_specs=(P("wlk", "pts"), P("wlk"), P("wlk")),
        check_vma=False,
    )
```

```python
import jax
import jax.numpy as jnp
from jax import lax
from jax.experimental import pallas as pl
from jax.experimental.pallas import tpu as pltpu
from jax.sharding import PartitionSpec as P

MESH = pl.DeviceIdType.MESH
F32, BF16 = jnp.float32, jnp.bfloat16

ELEC = 400
PTS = 600
PAD = 640
ROWS = 608
DEEP = 300
DEEP_PAD = 304
GROUPS = 8
C_CUT = 160
KCH = 160
CHUNK = ((0, 256), (256, 256), (512, 128))
PARTS = range(len(CHUNK))
STEPS = ((0, 2), (2, 4), (4, 5))
FLOWS = 110


def dot(a, b):
    return jnp.dot(a, b, preferred_element_type=F32)


def body(green, colloc, occ, kmat, pot_out, sum_out,
         cin, oin, gv, g8, kst, kb, cbuf, acc, ttown, ttbuf, tp, op, otown, otbuf,
         trans, dens, dbuf, ebuf, exch, pot, local_sem, send, recv, d_sem, e_sem, hear, pot_all):
    a, g = lax.axis_index("pts"), lax.axis_index("wlk")
    zh, x, c = a // 8, (a // 2) % 4, a % 2
    zl, y = g // 4, g % 4
    z = zh * 2 + zl
    is_same = zh == zl
    is_cross = zh != zl
    same = is_same.astype(jnp.int32)

    def at(zz, xx, cc, yy):
        return {"pts": (zz // 2) * 8 + xx * 2 + cc, "wlk": (zz % 2) * 4 + yy}

    sib = at(z, x, 1 - c, y)
    right, left = at(z, (x + 1) % 4, c, y), at(z, (x + 3) % 4, c, y)
    up, down = at(z, x, c, (y + 1) % 4), at(z, x, c, (y + 3) % 4)
    zmate = at(zh * 2 + 1 - zl, x, c, y)
    xmate = at(3 - z, x, c, y)
    lanes = tuple(pl.ds(pl.multiple_of(2 * start + c * size, 128), size) for start, size in CHUNK)
    cols = tuple(pl.ds(start, size) for start, size in CHUNK)
    numbers = iter(range(FLOWS))

    def flow(src, dst, dev, group):
        return pltpu.make_async_remote_copy(
            src_ref=src, dst_ref=dst, send_sem=send.at[group], recv_sem=recv.at[next(numbers)],
            device_id=dev, device_id_type=MESH)

    def sent(group, ref):
        pltpu.make_async_remote_copy(
            src_ref=ref, dst_ref=ref, send_sem=send.at[group], recv_sem=recv.at[0],
            device_id=sib, device_id_type=MESH).wait_send()

    def start(*copies):
        for cp in copies:
            cp.start()

    load_c = pltpu.make_async_copy(colloc, cin, local_sem.at[0])
    load_o = pltpu.make_async_copy(occ, oin, local_sem.at[1])
    load_g = [pltpu.make_async_copy(green.at[w], gv.at[pl.ds(w * ELEC, ELEC)], local_sem.at[2 + w]) for w in range(2)]
    pieces = [(s, min(KCH, PTS - s)) for s in range(0, PTS, KCH)]
    load_k = [pltpu.make_async_copy(kmat.at[pl.ds(s, n)], kst.at[i % 2, pl.ds(0, n)], local_sem.at[4 + i])
              for i, (s, n) in enumerate(pieces)]
    start(load_c, load_o)

    plane = z * 8 + x * 2 + c

    def plane_dev(r):
        q = (plane + r) % 32
        return at(q // 8, (q // 2) % 4, q % 2, y)

    barrier = pltpu.get_barrier_semaphore()
    for dev in (up, down, right, left, zmate, xmate, sib):
        pl.semaphore_signal(barrier, inc=1, device_id=dev, device_id_type=MESH)

    rounds = ((right, left), (right, left), (zmate, xmate), (sib,))

    def tell(r):
        for dev in rounds[r]:
            pl.semaphore_signal(hear.at[r], inc=1, device_id=dev, device_id_type=MESH)

    def heard(r):
        pl.semaphore_wait(hear.at[r], len(rounds[r]))
        if r + 1 < len(rounds):
            tell(r + 1)
    cbuf[g, :, pl.ds(PAD - 128, 128)] = jnp.zeros((DEEP_PAD, 128), BF16)
    cbuf[g, pl.ds(DEEP_PAD - 16, 16), :] = jnp.zeros((16, PAD), BF16)
    load_c.wait()
    cbuf[g, pl.ds(0, DEEP), pl.ds(0, PTS)] = cin[...]
    start(*load_g)
    load_o.wait()
    otown[:, pl.ds(PAD - 128, 128)] = jnp.zeros((ELEC, 128), BF16)
    otown[:, pl.ds(0, PTS)] = oin[...]

    @pl.when(is_same)
    def _():
        for h in PARTS:
            otbuf[0, :, lanes[h]] = otown[:, cols[h]]

    pl.semaphore_wait(barrier, 7)
    tell(0)

    def slot(zlo, yy):
        return zlo * 4 + yy

    def c_flow(group, k, h, dev, first=0, count=DEEP_PAD):
        ref = cbuf.at[k, pl.ds(first, count), cols[h]]
        return flow(ref, ref, dev, group)

    own_k, mate_k = slot(zl, y), slot(1 - zl, y)
    dn, un, on = (y + 3) % 4, (y + 1) % 4, (y + 2) % 4
    c_z, c_own, c_mate, c_far, c_zfar, c_matefar = [], [], [], [], [], []
    for h in PARTS:
        c_z.append(c_flow(0, own_k, h, zmate))
        c_own.append((c_flow(1, own_k, h, up), c_flow(1, own_k, h, down)))
        c_mate.append((c_flow(2, mate_k, h, up), c_flow(2, mate_k, h, down)))
        c_far.append((c_flow(3, slot(zl, dn), h, up, 0, C_CUT),
                      c_flow(3, slot(zl, un), h, down, C_CUT, DEEP_PAD - C_CUT)))
        if h == 0:
            c_zfar.append(c_flow(4, slot(zl, on), h, zmate))
        else:
            c_matefar.append((c_flow(5, slot(1 - zl, dn), h, up, 0, C_CUT),
                              c_flow(5, slot(1 - zl, un), h, down, C_CUT, DEEP_PAD - C_CUT)))
    start(*c_own[0], c_z[0], *c_own[1], c_z[1], c_z[2])

    def o_block(i, h):
        return otbuf.at[i, :, lanes[h]]

    o_xx = [flow(otown.at[:, cols[h]], o_block(0, h), xmate, 6) for h in PARTS]
    o_right = [flow(o_block(0, h), o_block(1, h), right, 7) for h in PARTS]
    o_left = [flow(o_block(0, h), o_block(2, h), left, 8) for h in PARTS]
    o_sib = [flow(o_block(0, h), o_block(0, h), sib, 9) for h in PARTS]
    o_far = [flow(o_block(1, 0), o_block(3, 0), right, 10), flow(o_block(2, 1), o_block(3, 1), left, 10),
             flow(o_block(1, 2), o_block(3, 2), right, 10)]
    o_relay = [[flow(o_block(i, h), o_block(i, h), sib, 11 + i // 3) for h in PARTS] for i in (1, 2, 3)]
    o_first = o_right + o_left + o_sib

    @pl.when(is_cross)
    def _():
        start(*o_xx)

    @pl.when(is_same)
    def _():
        for h in PARTS:
            start(o_right[h], o_left[h], o_sib[h])

    for cp in load_g:
        cp.wait()
    start(load_k[0], load_k[1])

    def cut_green(r, carry):
        rows = pl.ds(pl.multiple_of(r * 80, 16), 80)
        piece = gv[rows, :]
        for k in range(GROUPS):
            part = piece[:, k * DEEP:(k + 1) * DEEP]
            g8[k, rows, pl.ds(0, DEEP_PAD)] = jnp.concatenate([part, jnp.zeros((80, DEEP_PAD - DEEP), BF16)], axis=1)
        return carry

    lax.fori_loop(0, 10, cut_green, 0)
    heard(0)

    def add_theta(k, h, first=False):
        part = dot(g8[k, :, pl.ds(0, DEEP_PAD)], cbuf[k, :, cols[h]])
        if first:
            acc[:, cols[h]] = part
        else:
            acc[:, cols[h]] += part

    def cut_kernel(i):
        s, n = pieces[i]
        load_k[i].wait()

        def rows_at(r, carry):
            rows = pl.ds(pl.multiple_of(r * 16, 16), 16)
            out = pl.ds(pl.multiple_of(s + r * 16, 16), 16)
            for b in range(16):
                j, core = b // 2, b % 2
                kb[j, out, pl.ds(core * 256, 256)] = kst[i % 2, rows, pl.ds(b * PTS, 256)]
                kb[j, out, pl.ds(512 + core * 256, 256)] = kst[i % 2, rows, pl.ds(b * PTS + 256, 256)]
                part = kst[i % 2, rows, pl.ds(b * PTS + 512, PTS - 512)]
                kb[j, out, pl.ds(1024 + core * 128, 128)] = jnp.concatenate(
                    [part, jnp.zeros((16, PAD - PTS), BF16)], axis=1)
            return carry

        lax.fori_loop(0, (n + 15) // 16, rows_at, 0)
        if i + 2 < len(pieces):
            load_k[i + 2].start()

    def take(pair):
        for cp in pair:
            cp.wait_recv()

    def near_arrives(h):
        c_own[h][0].wait_recv()
        c_far[h][0].start()
        c_own[h][1].wait_recv()
        c_far[h][1].start()
        c_z[h].wait_recv()
        start(*c_mate[h])

    def far_arrives(h):
        take(c_far[h])
        if h == 0:
            c_zfar[0].start()

    for h in PARTS:
        add_theta(own_k, h, True)
    def occupied_part(h):
        o_right[h].wait_recv()
        o_left[h].wait_recv()
        start(o_far[h], o_relay[0][h], o_relay[1][h])

    def occupied_from_z(h):
        o_xx[h].wait_recv()
        start(o_right[h], o_left[h], o_sib[h])

    def add_near(h):
        add_theta(slot(zl, dn), h)
        add_theta(slot(zl, un), h)
        add_theta(mate_k, h)

    def add_mates(h):
        take(c_mate[h])
        if h:
            start(*c_matefar[h - 1])
        add_theta(slot(1 - zl, dn), h)
        add_theta(slot(1 - zl, un), h)

    cut_kernel(0)
    heard(1)
    near_arrives(0)
    start(*c_own[2])

    @pl.when(is_cross)
    def _():
        occupied_from_z(0)

    add_near(0)
    cut_kernel(1)
    near_arrives(1)

    @pl.when(is_cross)
    def _():
        occupied_from_z(1)

    far_arrives(0)

    @pl.when(is_same)
    def _():
        occupied_part(0)

    add_theta(slot(zl, on), 0)
    heard(2)
    add_near(1)

    @pl.when(is_cross)
    def _():
        occupied_from_z(2)

    @pl.when(is_same)
    def _():
        occupied_part(1)
        occupied_part(2)

    cut_kernel(3)
    add_mates(0)
    c_zfar[0].wait_recv()
    add_theta(slot(1 - zl, on), 0)

    def t_block(i, h):
        return ttbuf.at[i, :, lanes[h]]

    def t_flows(count, make):
        return [[make(w, h) for h in PARTS] for w in range(count)]

    t_z = t_flows(2, lambda w, h: flow(ttown.at[w, :, cols[h]], t_block(2 + w, h), zmate, 13))
    t_xx = t_flows(2, lambda w, h: flow(ttown.at[w, :, cols[h]], t_block(w, h), xmate, 14))
    t_sib = t_flows(2, lambda w, h: flow(t_block(w, h), t_block(w, h), sib, 15))
    t_sibz = t_flows(2, lambda w, h: flow(t_block(2 + w, h), t_block(2 + w, h), sib, 16))
    t_right = t_flows(2, lambda w, h: flow(t_block(w * (1 + same), h), t_block(4 + w, h), right, 17))
    t_left = t_flows(2, lambda w, h: flow(t_block(same + w * (1 + same), h), t_block(6 + w, h), left, 18))
    low_r = (x + 1) % 4 < 2
    low_l = (x + 3) % 4 < 2
    go_r = 4 + jnp.where(is_same & jnp.logical_not(low_r), 1, 0)
    go_l = 6 + jnp.where(is_same & low_l, 0, 1)
    t_far = [[flow(t_block(go_r, h), t_block(8, h), right, 19) for h in PARTS],
             [flow(t_block(go_l, h), t_block(9, h), left, 19) for h in PARTS]]
    t_relay = [[flow(t_block(i, h), t_block(i, h), sib, 20) for h in PARTS] for i in range(4, 10)]

    def turned(src, size):
        trans[pl.ds(0, ELEC), pl.ds(0, size)] = src.astype(F32)
        return jnp.swapaxes(trans[:, pl.ds(0, size)], 0, 1).astype(BF16)

    def turn(side, h):
        tp[side, cols[h], :] = turned(ttbuf[side, :, lanes[h]], CHUNK[h][1])

    def cross_go(w, h):
        t_xx[w][h].wait_recv()
        start(t_right[w][h], t_left[w][h], t_sib[w][h])

    def same_go(w, h):
        t_z[w][h].wait_recv()
        start(t_right[1][h] if w == 0 else t_left[1][h], t_sibz[w][h])
        turn(2 + w, h)

    def d_flow(r):
        return pltpu.make_async_remote_copy(
            src_ref=dbuf.at[a], dst_ref=dbuf.at[a], send_sem=d_sem.at[0], recv_sem=d_sem.at[1],
            device_id={"pts": (a + r) % 16, "wlk": g}, device_id_type=MESH)

    def d_start(r, carry):
        d_flow(r).start()
        return carry

    def d_wait():
        every = dbuf.at[pl.ds(0, 15)]
        pltpu.make_async_remote_copy(
            src_ref=every, dst_ref=every, send_sem=d_sem.at[0], recv_sem=d_sem.at[1],
            device_id=sib, device_id_type=MESH).wait()

    def publish(h):
        for w in range(2):
            t = acc[pl.ds(w * ELEC, ELEC), cols[h]].astype(BF16)
            ttown[w, :, cols[h]] = t

            @pl.when(is_same)
            def _():
                ttbuf[w, :, lanes[h]] = t

            dens[pl.ds(w, 1), cols[h]] = jnp.sum(
                t.astype(F32) * otown[:, cols[h]].astype(F32), axis=0, keepdims=True)

        if h == 2:
            dbuf[a] = dens[...].astype(BF16).astype(F32)
            lax.fori_loop(1, 16, d_start, 0)

        @pl.when(is_same)
        def _():
            start(t_right[0][h], t_left[0][h], t_z[0][h], t_sib[0][h], t_sib[1][h])
            if h == 2:
                start(*t_z[1])

        @pl.when(is_cross)
        def _():
            if h == 1:
                start(t_xx[0][1], t_z[0][1])
            elif h == 0:
                start(t_xx[0][0], t_z[0][0], t_xx[1][0], t_z[1][0])
            else:
                start(t_xx[1][1], t_z[1][1], t_xx[0][2], t_z[0][2], t_xx[1][2], t_z[1][2])

    publish(0)
    heard(3)

    near_arrives(2)
    far_arrives(1)

    @pl.when(is_cross)
    def _():
        occupied_part(0)

    @pl.when(is_cross)
    def _():
        occupied_part(1)

    add_theta(slot(zl, on), 1)
    cut_kernel(2)
    add_mates(1)
    far_arrives(2)

    @pl.when(is_cross)
    def _():
        occupied_part(2)

    add_near(2)
    add_theta(slot(zl, on), 2)

    @pl.when(is_cross)
    def _():
        cross_go(0, 0)

    add_mates(2)
    take(c_matefar[0])
    add_theta(slot(1 - zl, on), 1)
    publish(1)

    take(c_matefar[1])
    add_theta(slot(1 - zl, on), 2)
    publish(2)

    @pl.when(is_same)
    def _():
        same_go(0, 0)

    def potential(first):
        if first == 0:
            pot[...] = jnp.zeros_like(pot)

        def add_chip(j, carry):
            one, two = dbuf[2 * j].astype(BF16), dbuf[2 * j + 1].astype(BF16)
            both = jnp.concatenate([v[:, i:i + n] for i, n in CHUNK for v in (one, two)], axis=1)
            pot[...] += lax.dot_general(both, kb[j], (((1,), (1,)), ((), ())), preferred_element_type=F32)
            return carry

        lax.fori_loop(first, first + 4, add_chip, 0)
        if first:
            pot_all[...] = pot[:, pl.ds(0, PTS)]
            save_pot.start()

    save_pot = pltpu.make_async_copy(pot_all, pot_out, local_sem.at[0])
    exch[...] = jnp.zeros_like(exch)

    def unit(tt, side, ot, chip, weight, h):
        left_t = tp[side, pl.ds(0, ROWS), pl.ds(0, ELEC)]
        left_o = op[pl.ds(0, ROWS), pl.ds(0, ELEC)]

        def step(n, carry):
            part = pl.ds(n * 256, 256)
            near = dot(left_t, otbuf[ot, :, part])
            away = dot(left_o, ttbuf[tt, :, part])
            terms = kb[chip, :, part].astype(F32) * near * away
            return carry + terms.reshape(ROWS // 8, 8, 256).sum(axis=0)

        total = jnp.zeros((8, 256), F32)
        for n in range(*STEPS[h]):
            total = step(n, total)
        exch[side] += weight * total

    def z_take(w, h):
        t_z[w][h].wait_recv()
        turn(2 + w, h)

    def from_left(w, h):
        t_right[w][h].wait_recv()
        t_relay[w][h].start()

    def from_right(w, h):
        t_left[w][h].wait_recv()
        t_relay[2 + w][h].start()

    def from_both(w, h):
        from_left(w, h)
        from_right(w, h)

    def from_far(w, h):
        t_far[w][h].wait_recv()
        t_relay[4 + w][h].start()

    base = jnp.where(is_same, zh, 1 - zh) * 4
    of_same = {0: (0, 0, 0, 1.0), 1: (1, 0, 0, 1.0), 2: (2, 0, 0, 1.0), 3: (3, 0, 0, 1.0),
               4: (0, 1, 3, 2.0), 5: (2, 1, 3, 2.0), 6: (1, 2, 1, 2.0), 7: (3, 2, 1, 2.0),
               8: (2 * (x // 2), 3, 2, 2.0), 9: (2 * (x // 2) + 1, 3, 2, 2.0)}
    of_cross = {0: (2, 0, 0, 2.0), 1: (3, 0, 0, 2.0), 4: (2, 1, 3, 2.0), 5: (3, 1, 3, 2.0),
                6: (2, 2, 1, 2.0), 7: (3, 2, 1, 2.0), 8: (2, 3, 2, 2.0), 9: (3, 3, 2, 2.0)}

    def handed(i, h):
        return t_sib[i][h] if i < 2 else t_sibz[i - 2][h] if i < 4 else t_relay[i - 4][h]

    def run(s_block, x_block, h):
        @pl.when(is_same)
        def _():
            handed(s_block, h).wait_recv()

        @pl.when(is_cross)
        def _():
            handed(x_block, h).wait_recv()

        picked = [jnp.where(is_same, u, v) for u, v in zip((s_block, *of_same[s_block]), (x_block, *of_cross[x_block]))]
        unit(picked[0], picked[1], picked[2], base + (x + picked[3]) % 4, picked[4], h)

    def own(i, h):
        handed(i, h).wait_recv()
        side, ot, away, weight = of_same[i]
        unit(i, side, ot, base + (x + away) % 4, weight, h)

    op[...] = turned(otown[...], PAD)

    @pl.when(is_cross)
    def _():
        cross_go(1, 0)

    @pl.when(is_same)
    def _():
        same_go(1, 0)
        from_both(0, 0)

    kb[:, pl.ds(PTS, ROWS - PTS), :] = jnp.zeros((8, ROWS - PTS, 2 * PAD), BF16)
    take(o_sib)

    @pl.when(is_same)
    def _():
        for w in range(2):
            for h in PARTS:
                turn(w, h)
        own(0, 0)
        own(0, 1)
        own(0, 2)
        own(1, 0)
        same_go(0, 1)
        own(1, 1)
        own(1, 2)
        from_both(0, 1)

    @pl.when(is_cross)
    def _():
        z_take(0, 0)
        from_both(0, 0)
        cross_go(0, 1)
        z_take(0, 1)

    take(o_far)
    start(*o_relay[2])
    d_wait()
    potential(0)

    @pl.when(is_same)
    def _():
        same_go(1, 1)

    @pl.when(is_cross)
    def _():
        from_both(1, 0)
        cross_go(1, 1)
        start(t_far[0][0], t_far[1][0])
        z_take(0, 2)

    potential(4)
    for part in o_relay:
        take(part)
    run(4, 0, 0)
    run(4, 0, 1)

    @pl.when(is_same)
    def _():
        from_left(1, 0)
        t_far[0][0].start()
        same_go(0, 2)
        from_both(0, 2)
        from_right(1, 0)
        t_far[1][0].start()

    @pl.when(is_cross)
    def _():
        cross_go(0, 2)

    run(6, 4, 0)

    @pl.when(is_cross)
    def _():
        cross_go(1, 2)

    run(2, 6, 0)

    @pl.when(is_same)
    def _():
        same_go(1, 2)

    @pl.when(is_cross)
    def _():
        from_both(0, 1)
        t_far[0][1].start()

    run(4, 0, 2)

    @pl.when(is_same)
    def _():
        from_left(1, 1)
        t_far[0][1].start()

    run(6, 4, 1)

    @pl.when(is_cross)
    def _():
        z_take(1, 0)
        z_take(1, 1)

    run(2, 6, 1)

    @pl.when(is_same)
    def _():
        from_right(1, 1)
        t_far[1][1].start()

    @pl.when(is_cross)
    def _():
        z_take(1, 2)

    run(3, 1, 0)
    run(3, 1, 1)

    @pl.when(is_cross)
    def _():
        from_both(1, 1)
        t_far[1][1].start()

    run(5, 5, 0)
    run(7, 7, 0)

    run(6, 1, 2)
    from_far(0, 0)

    @pl.when(is_cross)
    def _():
        from_both(0, 2)
        t_far[0][2].start()

    @pl.when(is_same)
    def _():
        from_right(1, 2)
        t_far[1][2].start()

    run(5, 5, 1)

    @pl.when(is_same)
    def _():
        from_left(1, 2)
        t_far[0][2].start()

    run(8, 8, 0)
    from_far(1, 0)

    @pl.when(is_cross)
    def _():
        from_both(1, 2)
        t_far[1][2].start()

    run(7, 7, 1)
    run(9, 9, 0)
    run(2, 4, 2)
    run(3, 6, 2)
    run(5, 5, 2)
    from_far(0, 1)
    run(7, 7, 2)
    from_far(1, 1)
    run(8, 8, 1)
    from_far(0, 2)
    run(9, 9, 1)
    from_far(1, 2)
    run(8, 8, 2)
    run(9, 9, 2)

    lane = lax.broadcasted_iota(jnp.int32, (1, 128), 1)
    tile = jnp.zeros((1, 128), F32)
    for side in range(4):
        tile = jnp.where(lane == (zl * 2 + side) % 4, -0.5 * jnp.sum(exch[side]), tile)
    for w in range(2):
        tile = jnp.where(lane == 4 + zl * 2 + w,
                         0.5 * jnp.sum(dens[pl.ds(w, 1), pl.ds(0, PTS)] * pot[pl.ds(w, 1), pl.ds(0, PTS)]), tile)
    ebuf[plane] = tile

    def e_flow(r):
        return pltpu.make_async_remote_copy(
            src_ref=ebuf.at[plane], dst_ref=ebuf.at[plane], send_sem=e_sem.at[0], recv_sem=e_sem.at[1],
            device_id=plane_dev(r), device_id_type=MESH)

    for r in (*range(16, 32), *range(15, 0, -1)):
        e_flow(r).start()

    for group, ref in ((0, cbuf.at[0]), (1, cbuf.at[pl.ds(0, 2)]), (2, cbuf.at[pl.ds(0, 2)]), (3, cbuf.at[0]),
                       (4, cbuf.at[0, :, cols[0]]), (5, cbuf.at[0, :, pl.ds(256, 384)]),
                       (7, otown), (8, otown), (9, otown), (10, otown), (11, otbuf.at[0]), (12, otown),
                       (13, ttown), (15, ttown), (17, ttown), (18, ttown), (19, ttown), (20, ttbuf.at[pl.ds(0, 3)])):
        sent(group, ref)

    @pl.when(is_cross)
    def _():
        sent(6, otown)
        sent(14, ttown)

    @pl.when(is_same)
    def _():
        sent(16, ttown)

    save_pot.wait()
    every = ebuf.at[pl.ds(0, 31)]
    last = pltpu.make_async_remote_copy(
        src_ref=every, dst_ref=every, send_sem=e_sem.at[0], recv_sem=e_sem.at[1],
        device_id=sib, device_id_type=MESH)
    last.wait()
    sum_out[...] = ebuf[...].sum(axis=0)


def finish(pot, total, pot_out, cou_out, exc_out):
    zl = lax.axis_index("wlk") // 4
    pot_out[...] = pot[...]
    lane = lax.broadcasted_iota(jnp.int32, (1, 128), 1)
    for w in range(2):
        exc_out[w] = jnp.sum(jnp.where(lane == zl * 2 + w, total[...], 0.0))
        cou_out[w] = jnp.sum(jnp.where(lane == 4 + zl * 2 + w, total[...], 0.0))


def local(green_half, collocation, occupied, kernel):
    any_space = pl.BlockSpec(memory_space=pl.ANY)
    vmem = pltpu.VMEM
    in_vmem, in_smem = pl.BlockSpec(memory_space=vmem), pl.BlockSpec(memory_space=pltpu.SMEM)
    pot, total = pl.pallas_call(
        body,
        out_shape=(jax.ShapeDtypeStruct((2, PTS), F32), jax.ShapeDtypeStruct((1, 128), F32)),
        in_specs=[any_space] * 4,
        out_specs=(any_space, in_vmem),
        scratch_shapes=[
            vmem((DEEP, PTS), BF16),
            vmem((ELEC, PTS), BF16),
            vmem((2 * ELEC, 8 * DEEP), BF16),
            vmem((GROUPS, 2 * ELEC, 384), BF16),
            vmem((2, KCH, 16 * PTS), BF16),
            vmem((8, ROWS, 2 * PAD), BF16),
            vmem((GROUPS, DEEP_PAD, PAD), BF16),
            vmem((2 * ELEC, PAD), F32),
            vmem((2, ELEC, PAD), BF16),
            vmem((10, ELEC, 2 * PAD), BF16),
            vmem((4, PAD, 512), BF16),
            vmem((PAD, 512), BF16),
            vmem((ELEC, PAD), BF16),
            vmem((4, ELEC, 2 * PAD), BF16),
            vmem((512, PAD), F32),
            vmem((2, PAD), F32),
            vmem((16, 2, PAD), F32),
            vmem((32, 1, 128), F32),
            vmem((4, 8, 256), F32),
            vmem((2, ROWS), F32),
            pltpu.SemaphoreType.DMA((8,)),
            pltpu.SemaphoreType.DMA((21,)),
            pltpu.SemaphoreType.DMA((FLOWS,)),
            pltpu.SemaphoreType.DMA((2,)),
            pltpu.SemaphoreType.DMA((2,)),
            pltpu.SemaphoreType.REGULAR((4,)),
            vmem((2, PTS), F32),
        ],
        compiler_params=pltpu.CompilerParams(
            collective_id=0, has_side_effects=True, vmem_limit_bytes=67_000_000),
    )(green_half, collocation, occupied.T, kernel)
    return pl.pallas_call(
        finish,
        out_shape=(jax.ShapeDtypeStruct((2, PTS), F32), jax.ShapeDtypeStruct((2,), F32), jax.ShapeDtypeStruct((2,), F32)),
        in_specs=[in_vmem, in_vmem],
        out_specs=(in_vmem, in_smem, in_smem),
    )(pot, total)


def solution(mesh):
    placed = (P("wlk", None, None), P("wlk", "pts"), P("pts", None), P("pts", None))
    return jax.shard_map(
        local,
        mesh=mesh,
        in_specs=placed,
        out_specs=(P("wlk", "pts"), P("wlk"), P("wlk")),
        check_vma=False,
    )
```
